32 devices in a mesh: rows: 32 (over z, y, x, core).
Axes of the slice: x: 2, y: 2, z: 4, core: 2. Of those that a mesh axis runs over, the one named last changes fastest.
Arguments:
- wave_fn: float32 [512, 4, 4, 512], P('rows')
- left_env: bfloat16 [32, 512, 512], P(None, 'rows')
- op_pair: bfloat16 [32, 16, 16], replicated
- right_env: bfloat16 [32, 512, 512], replicated
Outputs:
- output 1: float32 [7, 512, 4, 4, 512], P(None, 'rows')
- output 2: float32 [6], replicated
- output 3: float32 [6], replicated
All inputs are finite; a program needn't handle non-finite values.
Results may differ from the reference program's by a relative error of at most 0.0119439.
Values are sent between devices in bfloat16 or wider.
A program may use at most 1 GiB of HBM per device.

```python
import jax
import jax.numpy as jnp
from jax import lax

BOND_DIM = 512
PHYS_DIM = 4
NUM_TERMS = 32
NUM_STEPS = 6


def sym_noise(rng_key, num_mats, mat_size):
    raw_draw = jax.random.normal(rng_key, (num_mats, mat_size, mat_size), jnp.float32)
    return (raw_draw + jnp.swapaxes(raw_draw, 1, 2)) * (0.5 ** 0.5) * mat_size ** -0.5


def setup_inputs(seed: int = 0) -> dict:
    key_list = jax.random.split(jax.random.key(seed), 7)
    pair_dim = PHYS_DIM * PHYS_DIM
    shift_left = jax.random.uniform(key_list[0], (NUM_TERMS, 1, 1), jnp.float32, 0.3, 0.9)
    shift_pair = jax.random.uniform(key_list[1], (NUM_TERMS, 1, 1), jnp.float32, 0.3, 0.9)
    shift_right = jax.random.uniform(key_list[2], (NUM_TERMS, 1, 1), jnp.float32, 0.3, 0.9)
    left_env = sym_noise(key_list[3], NUM_TERMS, BOND_DIM) + shift_left * jnp.eye(BOND_DIM, dtype=jnp.float32)
    op_pair = (sym_noise(key_list[4], NUM_TERMS, pair_dim) + shift_pair * jnp.eye(pair_dim, dtype=jnp.float32)) * NUM_TERMS ** -0.5
    right_env = sym_noise(key_list[5], NUM_TERMS, BOND_DIM) + shift_right * jnp.eye(BOND_DIM, dtype=jnp.float32)
    wave_fn = jax.random.normal(key_list[6], (BOND_DIM, PHYS_DIM, PHYS_DIM, BOND_DIM), jnp.float32)
    return {"wave_fn": wave_fn, "left_env": left_env.astype(jnp.bfloat16), "op_pair": op_pair.astype(jnp.bfloat16), "right_env": right_env.astype(jnp.bfloat16)}


def matvec(vec_in, left_env, op_pair, right_env):
    pair_dim = PHYS_DIM * PHYS_DIM
    flat_in = vec_in.astype(jnp.bfloat16).reshape(BOND_DIM, pair_dim * BOND_DIM)

    def add_term(acc_sum, term_ops):
        left_k, pair_k, right_k = term_ops
        left_out = jnp.dot(left_k, flat_in, preferred_element_type=jnp.float32).astype(jnp.bfloat16)
        left_out = left_out.reshape(BOND_DIM, pair_dim, BOND_DIM)
        mid_out = jnp.einsum("qr,arc->aqc", pair_k.astype(jnp.float32), left_out.astype(jnp.float32)).astype(jnp.bfloat16)
        part_out = jnp.dot(mid_out.reshape(BOND_DIM * pair_dim, BOND_DIM), right_k.T, preferred_element_type=jnp.float32)
        return acc_sum + part_out, None

    start_sum = jnp.zeros((BOND_DIM * pair_dim, BOND_DIM), jnp.float32)
    sigma_all = lax.scan(add_term, start_sum, (left_env, op_pair, right_env))[0]
    return sigma_all.reshape(BOND_DIM, PHYS_DIM, PHYS_DIM, BOND_DIM)


def reference(wave_fn, left_env, op_pair, right_env):
    vec_count = BOND_DIM * BOND_DIM * PHYS_DIM * PHYS_DIM
    first_vec = wave_fn / jnp.sqrt(jnp.sum(wave_fn * wave_fn) / vec_count)

    def lanczos_step(carry_in, unused):
        prev_vec, cur_vec, beta_prev = carry_in
        sigma_all = matvec(cur_vec, left_env, op_pair, right_env)
        alpha_val = jnp.sum(sigma_all * cur_vec) / vec_count
        resid_vec = sigma_all - alpha_val * cur_vec - beta_prev * prev_vec
        beta_val = jnp.sqrt(jnp.sum(resid_vec * resid_vec) / vec_count)
        next_vec = resid_vec / beta_val
        return (cur_vec, next_vec, beta_val), (next_vec, alpha_val, beta_val)

    start_carry = (jnp.zeros_like(first_vec), first_vec, jnp.zeros((), jnp.float32))
    later_vecs, alphas, betas = lax.scan(lanczos_step, start_carry, None, length=NUM_STEPS)[1]
    return jnp.concatenate([first_vec[None], later_vecs], axis=0), alphas, betas
```

```python
import functools

import jax
import jax.numpy as jnp
from jax import lax
from jax.experimental import pallas as pl
from jax.experimental.pallas import tpu as pltpu
from jax.sharding import PartitionSpec as P

NUM_STEPS = 6
MESH = pl.DeviceIdType.MESH
F32 = jnp.float32
BF16 = jnp.bfloat16


def lanczos_kernel(
    vec_count,
    psi_ref, left_ref, op_ref, right_ref,
    out_ref, alpha_ref, beta_ref,
    u_ref, stage_ref, env_l, env_r, kron_ref, x_ref, y_ref, sig_ref, part_ref, v_ref, w_ref, stat_ref,
    recv_sem, send_sem, pair_send, pair_recv, part_sem, stat_sem, load_sem, out_sem,
):
    idx = lax.axis_index("rows")
    core = lax.rem(idx, 2)
    pos_x = lax.rem(idx // 2, 2)
    pos_y = lax.rem(idx // 4, 2)
    pos_z = idx // 8
    chip = idx // 2
    sib = idx + 1 - 2 * core
    next_x = idx + 2 - 4 * pos_x
    next_y = idx + 4 - 8 * pos_y

    def block(cc, half, src):
        return u_ref.at[cc, pl.ds(4 * half, 4), pl.ds(pl.multiple_of(32 * src, 32), 32), :]

    def copy(cc, half, src, target, way):
        return pltpu.make_async_remote_copy(
            src_ref=block(cc, half, src), dst_ref=block(cc, half, src),
            send_sem=send_sem.at[way], recv_sem=recv_sem.at[src, 2 * cc + half],
            device_id=(target,), device_id_type=MESH)

    def arrived(cc, half, src):
        copy(cc, half, src, sib, 0).wait_recv()

    def chip_at(px, py, pz):
        return (pz * 2 + py) * 2 + px

    def send_x(cc, half, src):
        copy(cc, half, src, next_x, 0).start()

    def send_y(cc, half, src):
        copy(cc, half, src, next_y, 1).start()

    def send_up(cc, src):
        @pl.when(pos_z < 3)
        def _():
            for half in range(2):
                copy(cc, half, src, idx + 8, 2).start()

    def send_down(cc, src):
        @pl.when(pos_z > 0)
        def _():
            for half in range(2):
                copy(cc, half, src, idx - 8, 3).start()

    def at_distance(dist, act):
        if dist == 0:
            act(pos_z, 0)
            return

        @pl.when(pos_z >= dist)
        def _():
            act(pos_z - dist, 1)

        @pl.when(pos_z + dist <= 3)
        def _():
            act(pos_z + dist, -1)

    def own_z(cc):
        send_up(cc, chip)
        send_down(cc, chip)

    def column_xy(cc, dist):
        def act(pz, _):
            src = chip_at(pos_x, pos_y, pz)
            for half in range(2):
                send_x(cc, half, src)
                send_y(cc, half, src)
        at_distance(dist, act)

    def from_z(cc, dist):
        def act(pz, way):
            src = chip_at(pos_x, pos_y, pz)
            for half in range(2):
                arrived(cc, half, src)
            if way > 0:
                send_up(cc, src)
            else:
                send_down(cc, src)
        at_distance(dist, act)

    def from_xy(cc, dist):
        def act(pz, _):
            src_x = chip_at(1 - pos_x, pos_y, pz)
            src_y = chip_at(pos_x, 1 - pos_y, pz)
            arrived(cc, 0, src_x)
            send_y(cc, 0, src_x)
            arrived(cc, 1, src_y)
            send_x(cc, 1, src_y)
            arrived(cc, 1, src_x)
            arrived(cc, 0, src_y)
        at_distance(dist, act)

    def from_diag(cc):
        for pz in range(4):
            src = chip_at(1 - pos_x, 1 - pos_y, pz)
            for half in range(2):
                arrived(cc, half, src)

    def sends_done():
        def blocks(count):
            return u_ref.at[:, :, pl.ds(0, 32 * count), :]

        def wait(count, way):
            pltpu.make_async_copy(blocks(count), blocks(count), send_sem.at[way]).wait()

        wait(6, 0)
        wait(6, 1)
        for pz in range(4):
            @pl.when(pos_z == pz)
            def _():
                if pz < 3:
                    wait(pz + 1, 2)
                if pz > 0:
                    wait(4 - pz, 3)

    my_rows = pl.ds(pl.multiple_of(32 * chip + 16 * core, 16), 16)
    right_loads = [
        pltpu.make_async_copy(
            right_ref.at[:, pl.ds(pl.multiple_of(256 * core + 128 * cc, 128), 128), :], env_r.at[cc], load_sem.at[cc])
        for cc in range(2)]
    left_load = pltpu.make_async_copy(left_ref, env_l.at[:, core], load_sem.at[2])
    left_send = pltpu.make_async_remote_copy(
        src_ref=left_ref, dst_ref=env_l.at[:, core], send_sem=load_sem.at[3], recv_sem=load_sem.at[4],
        device_id=(sib,), device_id_type=MESH)
    left_send.start()
    left_load.start()
    for load in right_loads:
        load.start()

    def build_kron():
        row_id = lax.broadcasted_iota(jnp.int32, (256, 16), 0)
        col_id = lax.broadcasted_iota(jnp.int32, (256, 16), 1)
        spread = jnp.where(lax.shift_right_logical(row_id, 4) == col_id, 1.0, 0.0).astype(BF16)
        big_row = lax.broadcasted_iota(jnp.int32, (256, 256), 0)
        big_col = lax.broadcasted_iota(jnp.int32, (256, 256), 1)
        same = (big_row & 15) == (big_col & 15)

        def one(k, carry):
            tall = jnp.dot(spread, op_ref[k], preferred_element_type=F32).astype(BF16)
            full = lax.dot_general(tall, spread, (((1,), (1,)), ((), ())), preferred_element_type=F32)
            kron_ref[k] = jnp.where(same, full, 0.0).astype(BF16)
            return carry

        lax.fori_loop(0, 32, one, 0)

    def x_stage(cc):
        def one(rp, carry):
            out = jnp.dot(env_l[...].reshape(1024, 512), u_ref[cc, rp], preferred_element_type=F32)
            out = out.astype(BF16).reshape(32, 2, 16, 256)
            for ag in range(2):
                for par in range(2):
                    rows = pl.ds(pl.multiple_of((2 * rp + par) * 16, 16), 16)
                    x_ref[:, rows, ag * 128:(ag + 1) * 128] = out[:, ag, :, par * 128:(par + 1) * 128]
            return carry

        lax.fori_loop(0, 8, one, 0)

    def y_stage():
        def one(k4, carry):
            for kk in range(4):
                k = k4 * 4 + kk
                out = jnp.dot(kron_ref[k], x_ref[k], preferred_element_type=F32).astype(BF16)
                lanes = pl.ds(pl.multiple_of(k4 * 512 + kk * 128, 128), 128)
                for ag in range(2):
                    y_ref[ag, :, lanes] = out[:, ag * 128:(ag + 1) * 128]
            return carry

        lax.fori_loop(0, 8, one, 0)

    def s_stage(cc, ag):
        return jnp.dot(y_ref[ag], env_r[cc].reshape(4096, 512), preferred_element_type=F32)

    def exchange_stats():
        def stat_copy(target):
            return pltpu.make_async_remote_copy(
                src_ref=stat_ref.at[idx], dst_ref=stat_ref.at[idx], send_sem=stat_sem.at[0], recv_sem=stat_sem.at[1],
                device_id=(target,), device_id_type=MESH)

        def send(off, carry):
            stat_copy(lax.rem(idx + off, 32)).start()
            return carry

        lax.fori_loop(1, 32, send, 0)
        others = stat_ref.at[pl.ds(0, 31)]
        pltpu.make_async_copy(others, others, stat_sem.at[1]).wait()
        pltpu.make_async_copy(others, others, stat_sem.at[0]).wait()
        lane = lax.broadcasted_iota(jnp.int32, (1, 128), 1)

        def pick(row, which):
            return jnp.sum(jnp.where(lane == which, row, 0.0))

        rows = [stat_ref[d] for d in range(32)]
        total = rows[0]
        for row in rows[1:]:
            total = total + row
        alpha = pick(total, 0) / vec_count
        extra = jnp.zeros((1, 128), F32)
        for row in rows:
            delta = alpha - pltpu.roll(row, 2, 1)
            extra = extra + delta * (delta * row - 2.0 * pltpu.roll(row, 127, 1))
        beta_vec = jnp.sqrt(jnp.full((1, 128), (pick(total, 2) + pick(extra, 3)) / vec_count, F32))
        return alpha, jnp.max(beta_vec)

    def put_stats(dot_val, proj, sq_w, sq_v, cross):
        lane = lax.broadcasted_iota(jnp.int32, (1, 128), 1)
        row = jnp.zeros((1, 128), F32)
        for which, val in enumerate((dot_val, proj, sq_w, sq_v, cross)):
            row = jnp.where(lane == which, val, row)
        stat_ref[idx] = row

    def fold(val):
        return jnp.sum(val.reshape(2, 8, 512), axis=0)

    def normalise(slot, prev, alpha, beta, proj):
        delta = alpha - proj
        beta_row = jnp.full((1, 512), beta, F32)

        def one(q, carry):
            rows = pl.ds(pl.multiple_of(q * 16, 16), 16)
            v_ref[slot, rows, :] = (w_ref[rows, :] - delta * v_ref[prev, rows, :]) / beta_row
            return carry

        lax.fori_loop(0, 16, one, 0)

    def out_copy(step, slot):
        return pltpu.make_async_copy(v_ref.at[slot], out_ref.at[step], out_sem)

    zero_acc = jnp.zeros((8, 512), F32)

    def first(q, acc):
        rows = pl.ds(pl.multiple_of(q * 16, 16), 16)
        val = psi_ref[rows, :]
        w_ref[rows, :] = val
        v_ref[1, rows, :] = jnp.zeros((16, 512), F32)
        v_ref[2, rows, :] = jnp.zeros((16, 512), F32)
        return acc + fold(val * val)

    acc = lax.fori_loop(0, 16, first, zero_acc)
    put_stats(0.0, 0.0, jnp.sum(acc), 0.0, 0.0)

    def step_body(j, proj):
        cur = lax.rem(j, 3)
        prev = lax.rem(j + 2, 3)
        alpha, beta = exchange_stats()

        @pl.when(j > 0)
        def _():
            alpha_ref[j - 1] = alpha
            beta_ref[j - 1] = beta
            out_copy(j - 1, prev).wait()

        normalise(cur, prev, alpha, beta, proj)
        out_copy(j, cur).start()

        def to_bf16(rp, carry):
            for par in range(2):
                rows = pl.ds(pl.multiple_of((2 * rp + par) * 16, 16), 16)
                for cc in range(2):
                    own = pl.ds(pl.multiple_of(256 * core + 128 * cc, 128), 128)
                    far = pl.ds(pl.multiple_of(256 * (1 - core) + 128 * cc, 128), 128)
                    u_ref[cc, rp, my_rows, par * 128:(par + 1) * 128] = v_ref[cur, rows, own].astype(BF16)
                    stage_ref[cc, rp, :, par * 128:(par + 1) * 128] = v_ref[cur, rows, far].astype(BF16)
            return carry

        lax.fori_loop(0, 8, to_bf16, 0)

        def pair_copy(cc):
            return pltpu.make_async_remote_copy(
                src_ref=stage_ref.at[cc], dst_ref=u_ref.at[cc, :, my_rows, :],
                send_sem=pair_send.at[cc], recv_sem=pair_recv.at[cc], device_id=(sib,), device_id_type=MESH)

        for cc in range(2):
            pair_copy(cc).start()
        pair_copy(0).wait_recv()
        own_z(0)
        column_xy(0, 0)
        pair_copy(1).wait_recv()
        own_z(1)

        @pl.when(j == 0)
        def _():
            build_kron()

        from_z(0, 1)
        column_xy(0, 1)
        from_xy(0, 0)
        column_xy(1, 0)
        from_z(1, 1)
        from_z(0, 2)
        column_xy(0, 2)
        from_xy(0, 1)
        column_xy(1, 1)
        from_z(1, 2)
        from_z(0, 3)
        column_xy(0, 3)
        from_xy(0, 2)
        from_xy(1, 0)
        from_xy(0, 3)
        column_xy(1, 2)
        from_xy(1, 1)
        from_z(1, 3)
        column_xy(1, 3)
        from_xy(1, 2)
        from_diag(0)

        @pl.when(j == 0)
        def _():
            left_load.wait()
            left_send.wait()
            for load in right_loads:
                load.wait()

        x_stage(0)
        from_xy(1, 3)
        y_stage()
        sig_ref[0] = s_stage(0, 1 - core)
        sig_ref[1] = s_stage(0, core)
        from_diag(1)
        x_stage(1)
        y_stage()
        sig_ref[0] = sig_ref[0] + s_stage(1, 1 - core)
        part_copy = pltpu.make_async_remote_copy(
            src_ref=sig_ref.at[0], dst_ref=part_ref, send_sem=part_sem.at[0], recv_sem=part_sem.at[1],
            device_id=(sib,), device_id_type=MESH)
        part_copy.start()
        sig_ref[1] = sig_ref[1] + s_stage(1, core)
        part_copy.wait()
        for cc in range(2):
            pair_copy(cc).wait_send()
        sends_done()

        def dots(q, accs):
            rows = pl.ds(pl.multiple_of(q * 16, 16), 16)
            sig = sig_ref[1, rows, :] + part_ref[rows, :]
            vec = v_ref[cur, rows, :]
            w_ref[rows, :] = sig
            return accs[0] + fold(sig * vec), accs[1] + fold(vec * vec)

        acc_p, acc_v = lax.fori_loop(0, 16, dots, (zero_acc, zero_acc))
        dot_val = jnp.sum(acc_p)
        sq_v = jnp.sum(acc_v)
        proj_vec = jnp.full((1, 128), dot_val, F32) / jnp.full((1, 128), jnp.where(sq_v > 0.0, sq_v, 1.0), F32)
        new_proj = jnp.where(sq_v > 0.0, jnp.max(proj_vec), 0.0)
        beta_use = jnp.where(j > 0, beta, 0.0)

        def resid(q, accs):
            rows = pl.ds(pl.multiple_of(q * 16, 16), 16)
            vec = v_ref[cur, rows, :]
            res = w_ref[rows, :] - beta_use * v_ref[prev, rows, :] - new_proj * vec
            w_ref[rows, :] = res
            return accs[0] + fold(res * res), accs[1] + fold(res * vec)

        acc_w, acc_c = lax.fori_loop(0, 16, resid, (zero_acc, zero_acc))
        put_stats(dot_val, new_proj, jnp.sum(acc_w), sq_v, jnp.sum(acc_c))
        return new_proj

    proj = lax.fori_loop(0, NUM_STEPS, step_body, jnp.float32(0.0))
    alpha, beta = exchange_stats()
    alpha_ref[NUM_STEPS - 1] = alpha
    beta_ref[NUM_STEPS - 1] = beta
    out_copy(NUM_STEPS - 1, (NUM_STEPS - 1) % 3).wait()
    normalise(NUM_STEPS % 3, (NUM_STEPS - 1) % 3, alpha, beta, proj)
    last = out_copy(NUM_STEPS, NUM_STEPS % 3)
    last.start()
    last.wait()


def solution(mesh):
    def local_run(wave_rows, left_rows, op_pair, right_env):
        rows, phys, _, bond = wave_rows.shape
        pair = phys * phys
        vec_count = float(bond * bond * pair)
        psi = jnp.transpose(wave_rows.reshape(rows, pair, bond), (1, 0, 2)).reshape(pair * rows, bond)
        vecs, alpha, beta = pl.pallas_call(
            functools.partial(lanczos_kernel, vec_count),
            out_shape=(
                jax.ShapeDtypeStruct((NUM_STEPS + 1, pair * rows, bond), F32),
                jax.ShapeDtypeStruct((NUM_STEPS,), F32),
                jax.ShapeDtypeStruct((NUM_STEPS,), F32),
            ),
            in_specs=[
                pl.BlockSpec(memory_space=pltpu.VMEM),
                pl.BlockSpec(memory_space=pl.ANY),
                pl.BlockSpec(memory_space=pltpu.VMEM),
                pl.BlockSpec(memory_space=pl.ANY),
            ],
            out_specs=(
                pl.BlockSpec(memory_space=pl.ANY),
                pl.BlockSpec(memory_space=pltpu.SMEM),
                pl.BlockSpec(memory_space=pltpu.SMEM),
            ),
            scratch_shapes=[
                pltpu.VMEM((2, 8, 512, 256), BF16),
                pltpu.VMEM((2, 8, 16, 256), BF16),
                pltpu.VMEM((32, 2, 16, 512), BF16),
                pltpu.VMEM((2, 32, 128, 512), BF16),
                pltpu.VMEM((32, 256, 256), BF16),
                pltpu.VMEM((32, 256, 256), BF16),
                pltpu.VMEM((2, 256, 4096), BF16),
                pltpu.VMEM((2, 256, 512), F32),
                pltpu.VMEM((256, 512), F32),
                pltpu.VMEM((3, 256, 512), F32),
                pltpu.VMEM((256, 512), F32),
                pltpu.VMEM((32, 1, 128), F32),
                pltpu.SemaphoreType.DMA((16, 4)),
                pltpu.SemaphoreType.DMA((4,)),
                pltpu.SemaphoreType.DMA((2,)),
                pltpu.SemaphoreType.DMA((2,)),
                pltpu.SemaphoreType.DMA((2,)),
                pltpu.SemaphoreType.DMA((2,)),
                pltpu.SemaphoreType.DMA((5,)),
                pltpu.SemaphoreType.DMA,
            ],
            compiler_params=pltpu.CompilerParams(has_side_effects=True, vmem_limit_bytes=60 * 1024 * 1024),
        )(psi, left_rows, op_pair, right_env)
        vecs = vecs.reshape(NUM_STEPS + 1, pair, rows, bond).transpose(0, 2, 1, 3)
        return vecs.reshape(NUM_STEPS + 1, rows, phys, phys, bond), alpha, beta

    return jax.shard_map(
        local_run, mesh=mesh,
        in_specs=(P("rows"), P(None, "rows"), P(), P()),
        out_specs=(P(None, "rows"), P(), P()), check_vma=False)
```

```python
import functools

import jax
import jax.numpy as jnp
from jax import lax
from jax.experimental import pallas as pl
from jax.experimental.pallas import tpu as pltpu
from jax.sharding import PartitionSpec as P

NUM_STEPS = 6
MESH = pl.DeviceIdType.MESH
F32 = jnp.float32
BF16 = jnp.bfloat16

ROUTES = ("xzy", "yzx", "zyx", "zxy", "zxy", "zyx", "yxz", "zxy")
ORDER = (
    ("own", 2, "y", 0), ("own", 4, "x", 0), ("own", 2, "z", 0), ("own", 0, "x", 0), ("own", 0, "z", 0),
    ("own", 0, "y", 0), ("own", 1, "y", 0), ("own", 3, "y", 0), ("own", 3, "z", 0), ("own", 3, "x", 0),
    ("own", 2, "x", 0), ("own", 1, "z", 0), ("ev", 2, 0, 1), ("ev", 0, 1, 0), ("ev", 4, 1, 0), ("ev", 0, 0, 1),
    ("ev", 3, 0, 1), ("ev", 1, 2, 0), ("ev", 1, 0, 1), ("ev", 0, 1, 1), ("own", 4, "y", 0), ("own", 5, "x", 0),
    ("own", 1, "x", 0), ("ev", 2, 2, 0), ("ev", 0, 0, 2), ("ev", 3, 0, 2), ("ev", 2, 2, 1), ("ev", 1, 0, 2),
    ("ev", 2, 0, 2), ("own", 4, "z", 0), ("own", 6, "y", 0), ("ev", 0, 1, 2), ("ev", 1, 2, 1), ("ev", 3, 1, 2),
    ("own", 5, "z", 0), ("ev", 3, 1, 1), ("ev", 1, 0, 3), ("own", 7, "z", 0), ("ev", 0, 0, 3), ("ev", 3, 0, 3),
    ("own", 6, "x", 0), ("ev", 2, 0, 3), ("ev", 2, 3, 1), ("ev", 0, 2, 0), ("ev", 0, 3, 1), ("ev", 0, 3, 0),
    ("own", 6, "z", 0), ("ev", 1, 2, 2), ("own", 7, "x", 0), ("ev", 0, 1, 3), ("ev", 0, 2, 2), ("ev", 1, 1, 3),
    ("ev", 3, 1, 0), ("ev", 4, 0, 1), ("ev", 0, 3, 2), ("ev", 6, 0, 1), ("ev", 1, 1, 1), ("own", 5, "y", 0),
    ("ev", 0, 2, 1), ("ev", 0, 2, 3), ("ev", 2, 2, 2), ("own", 7, "y", 0), ("ev", 1, 3, 0), ("ev", 2, 1, 2),
    ("ev", 1, 3, 1), ("ev", 1, 2, 3), ("ev", 3, 2, 3), ("ev", 2, 1, 0), ("ev", 1, 1, 0), ("ev", 6, 2, 0),
    ("ev", 3, 2, 2), ("ev", 5, 0, 1), ("ev", 2, 2, 3), ("ev", 0, 3, 3), ("ev", 3, 1, 3), ("ev", 4, 0, 2),
    ("ev", 1, 3, 2), ("ev", 3, 2, 1), ("ev", 7, 0, 1), ("ev", 1, 3, 3), ("ev", 4, 0, 3), ("ev", 2, 1, 1),
    ("ev", 4, 3, 0), ("ev", 3, 3, 1), ("ev", 6, 0, 2), ("ev", 6, 1, 0), ("ev", 1, 1, 2), ("left", 1, 0, 0),
    ("ev", 7, 1, 0), ("ev", 2, 3, 0), ("ev", 3, 3, 2), ("ev", 3, 3, 3), ("ev", 2, 1, 3), ("ev", 7, 0, 2),
    ("ev", 2, 3, 2), ("ev", 2, 3, 3), ("ev", 3, 3, 0), ("left", 0, 0, 0), ("ev", 5, 0, 2), ("ev", 5, 2, 0),
    ("ev", 3, 2, 0), ("ev", 6, 2, 1), ("left", 3, 0, 0), ("ev", 7, 0, 3), ("left", 2, 0, 0), ("ev", 5, 0, 3),
    ("ev", 6, 3, 0), ("ev", 6, 1, 1), ("mid", 0, 0, 0), ("ev", 6, 0, 3), ("ev", 7, 1, 1), ("ev", 5, 2, 1),
    ("ev", 6, 2, 2), ("ev", 4, 1, 3), ("mid", 1, 0, 0), ("ev", 4, 1, 2), ("mid", 2, 0, 0), ("ev", 7, 2, 1),
    ("mid", 3, 0, 0), ("ev", 5, 1, 0), ("ev", 4, 1, 1), ("ev", 6, 3, 1), ("ev", 5, 2, 2), ("ev", 7, 1, 3),
    ("ev", 5, 1, 2), ("ev", 5, 2, 3), ("ev", 7, 1, 2), ("ev", 7, 2, 3), ("ev", 5, 1, 1), ("ev", 6, 1, 2),
    ("ev", 4, 2, 3), ("right", 0, 0, 0), ("ev", 7, 3, 0), ("ev", 5, 3, 0), ("ev", 6, 3, 2), ("right", 1, 0, 0),
    ("ev", 5, 3, 1), ("ev", 5, 3, 2), ("ev", 4, 3, 2), ("ev", 4, 2, 0), ("ev", 4, 2, 1), ("ev", 7, 2, 2),
    ("ev", 7, 2, 0), ("ev", 6, 1, 3), ("ev", 4, 2, 2), ("ev", 5, 3, 3), ("ev", 5, 1, 3), ("left", 5, 0, 0),
    ("ev", 7, 3, 1), ("ev", 4, 3, 3), ("ev", 7, 3, 3), ("ev", 4, 3, 1), ("left", 4, 0, 0), ("ev", 7, 3, 2),
    ("left", 7, 0, 0), ("ev", 6, 2, 3), ("ev", 6, 3, 3), ("left", 6, 0, 0), ("mid", 4, 0, 0), ("mid", 5, 0, 0),
    ("mid", 6, 0, 0), ("mid", 7, 0, 0), ("right", 2, 0, 0), ("right", 3, 0, 0),
)


def onward(route, cls, dist):
    if route[0] == "z":
        first, second = route[1], route[2]
    elif route[2] == "z":
        first, second = route[0], route[1]
    else:
        first, second = route[0], route[2]
    bit = {"x": 1, "y": 2}
    off_first, off_second = bool(cls & bit[first]), bool(cls & bit[second])
    if route[0] == "z":
        if cls == 0:
            return ["z", first, second]
        return [second] if off_first and not off_second else []
    if route[2] == "z":
        ways = []
        if dist == 0 and cls == 0:
            ways = [first, second]
        elif dist == 0 and off_first and not off_second:
            ways = [second]
        return ways + ["z"]
    if off_second:
        return []
    return ([first] if dist == 0 and not off_first else []) + [second, "z"]


def sends_on(way, cc, pz):
    count = 0
    for piece in range(4 * cc, 4 * cc + 4):
        for cls in range(4):
            for src_z in range(4):
                ways = onward(ROUTES[piece], cls, abs(pz - src_z))
                if way in ("x", "y"):
                    count += way in ways
                elif way == "up":
                    count += "z" in ways and src_z <= pz < 3
                else:
                    count += "z" in ways and src_z >= pz > 0
    return count


def lanczos_kernel(
    vec_count,
    psi_ref, left_ref, op_ref, right_ref,
    out_ref, alpha_ref, beta_ref,
    u_ref, stage_ref, env_l, env_r, kron_ref, x_ref, y_ref, sig_ref, part_ref, v_ref, w_ref, stat_ref,
    recv_sem, send_sem, pair_send, pair_recv, part_sem, stat_sem, load_sem, out_sem,
):
    idx = lax.axis_index("rows")
    core = lax.rem(idx, 2)
    pos_x = lax.rem(idx // 2, 2)
    pos_y = lax.rem(idx // 4, 2)
    pos_z = idx // 8
    chip = idx // 2
    sib = idx + 1 - 2 * core
    next_x = idx + 2 - 4 * pos_x
    next_y = idx + 4 - 8 * pos_y

    def block(piece, first_row, rows):
        return u_ref.at[piece // 4, pl.ds(2 * (piece % 4), 2), pl.ds(pl.multiple_of(first_row, 16), rows), :]

    WAYS = {"x": 0, "y": 1, "up": 2, "down": 3}

    def copy(piece, src, way, first_row, rows):
        target = {"x": next_x, "y": next_y, "up": idx + 8, "down": idx - 8}[way]
        ref = block(piece, first_row, rows)
        return pltpu.make_async_remote_copy(
            src_ref=ref, dst_ref=ref, send_sem=send_sem.at[WAYS[way] + 4 * (piece // 4)],
            recv_sem=recv_sem.at[src, piece], device_id=(target,), device_id_type=MESH)

    def send(piece, src, way, first_row=None, rows=32):
        if first_row is None:
            first_row = 32 * src
        if way == "up":
            @pl.when(pos_z < 3)
            def _():
                copy(piece, src, way, first_row, rows).start()
        elif way == "down":
            @pl.when(pos_z > 0)
            def _():
                copy(piece, src, way, first_row, rows).start()
        else:
            copy(piece, src, way, first_row, rows).start()

    def send_own(piece, way, first_row=None, rows=32):
        for one in (("up", "down") if way == "z" else (way,)):
            send(piece, chip, one, first_row, rows)

    def arrival(piece, cls, dist):
        col_x = 1 - pos_x if cls & 1 else pos_x
        col_y = 1 - pos_y if cls & 2 else pos_y

        def act(src_z, heading):
            src = (src_z * 2 + col_y) * 2 + col_x
            copy(piece, src, "x", 32 * src, 32).wait_recv()
            for way in onward(ROUTES[piece], cls, dist):
                if way != "z":
                    send(piece, src, way)
                else:
                    for one in heading:
                        send(piece, src, one)

        if dist == 0:
            act(pos_z, ("up", "down"))
            return

        @pl.when(pos_z >= dist)
        def _():
            act(pos_z - dist, ("up",))

        @pl.when(pos_z + dist <= 3)
        def _():
            act(pos_z + dist, ("down",))

    def sends_done():
        def wait(count, way, cc):
            if count:
                ref = env_r.at[0, pl.ds(0, count), pl.ds(0, 32), :]
                pltpu.make_async_copy(ref, ref, send_sem.at[WAYS[way] + 4 * cc]).wait()

        for cc in range(2):
            wait(sends_on("x", cc, 0), "x", cc)
            wait(sends_on("y", cc, 0), "y", cc)
        for pz in range(4):
            @pl.when(pos_z == pz)
            def _():
                for cc in range(2):
                    wait(sends_on("up", cc, pz), "up", cc)
                    wait(sends_on("down", cc, pz), "down", cc)

    my_rows = pl.ds(pl.multiple_of(32 * chip + 16 * core, 16), 16)
    right_loads = [
        pltpu.make_async_copy(
            right_ref.at[:, pl.ds(pl.multiple_of(256 * core + 128 * cc, 128), 128), :], env_r.at[cc], load_sem.at[cc])
        for cc in range(2)]
    left_load = pltpu.make_async_copy(left_ref, env_l.at[:, core], load_sem.at[2])
    left_send = pltpu.make_async_remote_copy(
        src_ref=left_ref, dst_ref=env_l.at[:, core], send_sem=load_sem.at[3], recv_sem=load_sem.at[4],
        device_id=(sib,), device_id_type=MESH)
    left_send.start()
    left_load.start()
    for load in right_loads:
        load.start()

    def build_kron():
        row_id = lax.broadcasted_iota(jnp.int32, (256, 16), 0)
        col_id = lax.broadcasted_iota(jnp.int32, (256, 16), 1)
        spread = jnp.where(lax.shift_right_logical(row_id, 4) == col_id, 1.0, 0.0).astype(BF16)
        big_row = lax.broadcasted_iota(jnp.int32, (256, 256), 0)
        big_col = lax.broadcasted_iota(jnp.int32, (256, 256), 1)
        same = (big_row & 15) == (big_col & 15)

        def one(k, carry):
            tall = jnp.dot(spread, op_ref[k], preferred_element_type=F32).astype(BF16)
            full = lax.dot_general(tall, spread, (((1,), (1,)), ((), ())), preferred_element_type=F32)
            kron_ref[k] = jnp.where(same, full, 0.0).astype(BF16)
            return carry

        lax.fori_loop(0, 32, one, 0)

    def left_part(piece):
        for sub in range(2):
            rp = 2 * (piece % 4) + sub
            out = jnp.dot(env_l[...].reshape(1024, 512), u_ref[piece // 4, rp], preferred_element_type=F32)
            out = out.astype(BF16).reshape(32, 2, 16, 256)
            for ag in range(2):
                for par in range(2):
                    row = (2 * rp + par) * 16
                    x_ref[:, row:row + 16, ag * 128:(ag + 1) * 128] = out[:, ag, :, par * 128:(par + 1) * 128]

    def mid_part(part):
        for kk in range(8):
            k = 8 * (part % 4) + kk
            out = jnp.dot(kron_ref[k], x_ref[k], preferred_element_type=F32).astype(BF16)
            for ag in range(2):
                y_ref[ag, :, k * 128:(k + 1) * 128] = out[:, ag * 128:(ag + 1) * 128]

    def right_part(part):
        cc, who = part // 2, part % 2
        ag = 1 - core if who == 0 else core
        out = jnp.dot(y_ref[ag], env_r[cc].reshape(4096, 512), preferred_element_type=F32)
        sig_ref[who] = out if cc == 0 else sig_ref[who] + out

    def exchange_stats():
        def stat_copy(target):
            return pltpu.make_async_remote_copy(
                src_ref=stat_ref.at[idx], dst_ref=stat_ref.at[idx], send_sem=stat_sem.at[0], recv_sem=stat_sem.at[1],
                device_id=(target,), device_id_type=MESH)

        def to_all(off, carry):
            stat_copy(lax.rem(idx + off, 32)).start()
            return carry

        lax.fori_loop(1, 32, to_all, 0)
        others = stat_ref.at[pl.ds(0, 31)]
        pltpu.make_async_copy(others, others, stat_sem.at[1]).wait()
        pltpu.make_async_copy(others, others, stat_sem.at[0]).wait()
        lane = lax.broadcasted_iota(jnp.int32, (1, 128), 1)

        def pick(row, which):
            return jnp.sum(jnp.where(lane == which, row, 0.0))

        rows = [stat_ref[d] for d in range(32)]
        total = rows[0]
        for row in rows[1:]:
            total = total + row
        alpha = pick(total, 0) / vec_count
        extra = jnp.zeros((1, 128), F32)
        for row in rows:
            delta = alpha - pltpu.roll(row, 2, 1)
            extra = extra + delta * (delta * row - 2.0 * pltpu.roll(row, 127, 1))
        beta_vec = jnp.sqrt(jnp.full((1, 128), (pick(total, 2) + pick(extra, 3)) / vec_count, F32))
        return alpha, jnp.max(beta_vec)

    def put_stats(dot_val, proj, sq_w, sq_v, cross):
        lane = lax.broadcasted_iota(jnp.int32, (1, 128), 1)
        row = jnp.zeros((1, 128), F32)
        for which, val in enumerate((dot_val, proj, sq_w, sq_v, cross)):
            row = jnp.where(lane == which, val, row)
        stat_ref[idx] = row

    def fold(val):
        return jnp.sum(val.reshape(2, 8, 512), axis=0)

    def normalise(slot, prev, alpha, beta, proj):
        delta = alpha - proj
        beta_row = jnp.full((1, 512), beta, F32)

        def one(q, carry):
            rows = pl.ds(pl.multiple_of(q * 16, 16), 16)
            vec = (w_ref[rows, :] - delta * v_ref[prev, rows, :]) / beta_row
            v_ref[slot, rows, :] = vec
            return carry + fold(vec * vec)

        return lax.fori_loop(0, 16, one, jnp.zeros((8, 512), F32))

    def out_copy(step, slot):
        return pltpu.make_async_copy(v_ref.at[slot], out_ref.at[step], out_sem)

    zero_acc = jnp.zeros((8, 512), F32)

    def first(q, acc):
        rows = pl.ds(pl.multiple_of(q * 16, 16), 16)
        val = psi_ref[rows, :]
        w_ref[rows, :] = val
        v_ref[1, rows, :] = jnp.zeros((16, 512), F32)
        v_ref[2, rows, :] = jnp.zeros((16, 512), F32)
        return acc + fold(val * val)

    acc = lax.fori_loop(0, 16, first, zero_acc)
    put_stats(0.0, 0.0, jnp.sum(acc), 0.0, 0.0)

    def step_body(j, proj):
        cur = lax.rem(j, 3)
        prev = lax.rem(j + 2, 3)
        alpha, beta = exchange_stats()

        @pl.when(j > 0)
        def _():
            alpha_ref[j - 1] = alpha
            beta_ref[j - 1] = beta
            out_copy(j - 1, prev).wait()

        acc_v = normalise(cur, prev, alpha, beta, proj)
        out_copy(j, cur).start()

        def to_bf16(rp, carry):
            for par in range(2):
                rows = pl.ds(pl.multiple_of((2 * rp + par) * 16, 16), 16)
                for cc in range(2):
                    own = pl.ds(pl.multiple_of(256 * core + 128 * cc, 128), 128)
                    far = pl.ds(pl.multiple_of(256 * (1 - core) + 128 * cc, 128), 128)
                    u_ref[cc, rp, my_rows, par * 128:(par + 1) * 128] = v_ref[cur, rows, own].astype(BF16)
                    stage_ref[cc, rp, :, par * 128:(par + 1) * 128] = v_ref[cur, rows, far].astype(BF16)
            return carry

        lax.fori_loop(0, 8, to_bf16, 0)

        def pair_copy(cc):
            return pltpu.make_async_remote_copy(
                src_ref=stage_ref.at[cc], dst_ref=u_ref.at[cc, :, my_rows, :],
                send_sem=pair_send.at[cc], recv_sem=pair_recv.at[cc], device_id=(sib,), device_id_type=MESH)

        for cc in range(2):
            pair_copy(cc).start()
        lead = 0
        while ORDER[lead][0] == "own":
            lead += 1
        for _, piece, way, _ in ORDER[:lead]:
            send_own(piece, way, 32 * chip + 16 * core, 16)
        for cc in range(2):
            pair_copy(cc).wait_recv()
            for _, piece, way, _ in ORDER[:lead]:
                if piece // 4 == cc:
                    send_own(piece, way, 32 * chip + 16 * (1 - core), 16)
        sq_v = jnp.sum(acc_v)

        @pl.when(j == 0)
        def _():
            build_kron()
            left_load.wait()
            left_send.wait()
            for load in right_loads:
                load.wait()

        part_copy = pltpu.make_async_remote_copy(
            src_ref=sig_ref.at[0], dst_ref=part_ref, send_sem=part_sem.at[0], recv_sem=part_sem.at[1],
            device_id=(sib,), device_id_type=MESH)
        for what, first_arg, second_arg, third_arg in ORDER[lead:]:
            if what == "own":
                send_own(first_arg, second_arg)
            elif what == "ev":
                arrival(first_arg, second_arg, third_arg)
            elif what == "left":
                left_part(first_arg)
            elif what == "mid":
                mid_part(first_arg)
            else:
                right_part(first_arg)
                if first_arg == 2:
                    part_copy.start()
        part_copy.wait()
        for cc in range(2):
            pair_copy(cc).wait_send()
        sends_done()

        def dots(q, accs):
            rows = pl.ds(pl.multiple_of(q * 16, 16), 16)
            sig = sig_ref[1, rows, :] + part_ref[rows, :]
            vec = v_ref[cur, rows, :]
            w_ref[rows, :] = sig
            return accs + fold(sig * vec)

        dot_val = jnp.sum(lax.fori_loop(0, 16, dots, zero_acc))
        proj_vec = jnp.full((1, 128), dot_val, F32) / jnp.full((1, 128), jnp.where(sq_v > 0.0, sq_v, 1.0), F32)
        new_proj = jnp.where(sq_v > 0.0, jnp.max(proj_vec), 0.0)
        beta_use = jnp.where(j > 0, beta, 0.0)

        def resid(q, accs):
            rows = pl.ds(pl.multiple_of(q * 16, 16), 16)
            vec = v_ref[cur, rows, :]
            res = w_ref[rows, :] - beta_use * v_ref[prev, rows, :] - new_proj * vec
            w_ref[rows, :] = res
            return accs[0] + fold(res * res), accs[1] + fold(res * vec)

        acc_w, acc_c = lax.fori_loop(0, 16, resid, (zero_acc, zero_acc))
        put_stats(dot_val, new_proj, jnp.sum(acc_w), sq_v, jnp.sum(acc_c))
        return new_proj

    proj = lax.fori_loop(0, NUM_STEPS, step_body, jnp.float32(0.0))
    alpha, beta = exchange_stats()
    alpha_ref[NUM_STEPS - 1] = alpha
    beta_ref[NUM_STEPS - 1] = beta
    out_copy(NUM_STEPS - 1, (NUM_STEPS - 1) % 3).wait()
    normalise(NUM_STEPS % 3, (NUM_STEPS - 1) % 3, alpha, beta, proj)
    last = out_copy(NUM_STEPS, NUM_STEPS % 3)
    last.start()
    last.wait()


def solution(mesh):
    def local_run(wave_rows, left_rows, op_pair, right_env):
        rows, phys, _, bond = wave_rows.shape
        pair = phys * phys
        vec_count = float(bond * bond * pair)
        psi = jnp.transpose(wave_rows.reshape(rows, pair, bond), (1, 0, 2)).reshape(pair * rows, bond)
        vecs, alpha, beta = pl.pallas_call(
            functools.partial(lanczos_kernel, vec_count),
            out_shape=(
                jax.ShapeDtypeStruct((NUM_STEPS + 1, pair * rows, bond), F32),
                jax.ShapeDtypeStruct((NUM_STEPS,), F32),
                jax.ShapeDtypeStruct((NUM_STEPS,), F32),
            ),
            in_specs=[
                pl.BlockSpec(memory_space=pltpu.VMEM),
                pl.BlockSpec(memory_space=pl.ANY),
                pl.BlockSpec(memory_space=pltpu.VMEM),
                pl.BlockSpec(memory_space=pl.ANY),
            ],
            out_specs=(
                pl.BlockSpec(memory_space=pl.ANY),
                pl.BlockSpec(memory_space=pltpu.SMEM),
                pl.BlockSpec(memory_space=pltpu.SMEM),
            ),
            scratch_shapes=[
                pltpu.VMEM((2, 8, 512, 256), BF16),
                pltpu.VMEM((2, 8, 16, 256), BF16),
                pltpu.VMEM((32, 2, 16, 512), BF16),
                pltpu.VMEM((2, 32, 128, 512), BF16),
                pltpu.VMEM((32, 256, 256), BF16),
                pltpu.VMEM((32, 256, 256), BF16),
                pltpu.VMEM((2, 256, 4096), BF16),
                pltpu.VMEM((2, 256, 512), F32),
                pltpu.VMEM((256, 512), F32),
                pltpu.VMEM((3, 256, 512), F32),
                pltpu.VMEM((256, 512), F32),
                pltpu.VMEM((32, 1, 128), F32),
                pltpu.SemaphoreType.DMA((16, 8)),
                pltpu.SemaphoreType.DMA((8,)),
                pltpu.SemaphoreType.DMA((2,)),
                pltpu.SemaphoreType.DMA((2,)),
                pltpu.SemaphoreType.DMA((2,)),
                pltpu.SemaphoreType.DMA((2,)),
                pltpu.SemaphoreType.DMA((5,)),
                pltpu.SemaphoreType.DMA,
            ],
            compiler_params=pltpu.CompilerParams(has_side_effects=True, vmem_limit_bytes=60 * 1024 * 1024),
        )(psi, left_rows, op_pair, right_env)
        vecs = vecs.reshape(NUM_STEPS + 1, pair, rows, bond).transpose(0, 2, 1, 3)
        return vecs.reshape(NUM_STEPS + 1, rows, phys, phys, bond), alpha, beta

    return jax.shard_map(
        local_run, mesh=mesh,
        in_specs=(P("rows"), P(None, "rows"), P(), P()),
        out_specs=(P(None, "rows"), P(), P()), check_vma=False)
```

```python
import functools

import jax
import jax.numpy as jnp
from jax import lax
from jax.experimental import pallas as pl
from jax.experimental.pallas import tpu as pltpu
from jax.sharding import PartitionSpec as P

NUM_STEPS = 6
MESH = pl.DeviceIdType.MESH
F32 = jnp.float32
BF16 = jnp.bfloat16

ROUTES = ("xzy", "yzx", "zyx", "zxy", "zxy", "zyx", "yxz", "zxy")
ORDER = (
    "o1y", "o1x", "o5y", "o3z", "o5x", "o6y", "o7z", "o0x", "o3y", "o2x", "o2z", "o4z", "o4y", "o3x", "o1z", "o0y",
    "o0z", "o7y", "o6x", "e3n1", "e1y0", "o2y", "e2n1", "e0x0", "e0n1", "e1n1", "e3n2", "e2n2", "e1x0", "e4y0",
    "e6y0", "e7n1", "e2y0", "e0n2", "e1y1", "e2x0", "e2y1", "e3y1", "e0x1", "e3x1", "e3n3", "e6x0", "e3x0", "e3x2",
    "e2y2", "e1n2", "e7n2", "e0x2", "e2d0", "e0y1", "o7x", "o5z", "e3x3", "e2n3", "e1x1", "e4n1", "e1n3", "e7n3",
    "e3d3", "e0y0", "e1d0", "e1y2", "e0d1", "e3y2", "e6d0", "o6z", "e2d1", "e0x3", "e2y3", "e2x3", "e4n2", "e0n3",
    "e1d1", "e2d2", "e7y0", "e7y3", "e2x2", "e5n1", "o4x", "e0d3", "e7x3", "e0d0", "e3y0", "e1y3", "e4n3", "e5n2",
    "e2x1", "e2d3", "l2", "e6y1", "e6n1", "e5n3", "e5x0", "e6x1", "e1d2", "e3d1", "e0d2", "e3d0", "e3d2", "e3y3",
    "e1x2", "e7x0", "e6d1", "l3", "e0y3", "e0y2", "e1x3", "e6y2", "e7x2", "e5y0", "e7x1", "l0", "e1d3", "e6n2", "l1",
    "e5y1", "e6x2", "e4y2", "e4x2", "e5y2", "e4x3", "m0", "e4x0", "e4x1", "m1", "m2", "e4y3", "m3", "e6d2", "e5y3",
    "e7y1", "r0", "r1", "e7d0", "e6x3", "e5x1", "e6d3", "e7d2", "e6y3", "e7d1", "e6n3", "e5x3", "e5d2", "e7d3",
    "e7y2", "l6", "e4d3", "l7", "e5d3", "e5x2", "e4d2", "e4d0", "e5d1", "e5d0", "l5", "e4d1", "e4y1", "l4", "m4",
    "m5", "m6", "m7", "r2", "r3",
)


CLASSES = "nxyd"


def onward(route, cls, dist):
    if route[0] == "z":
        first, second = route[1], route[2]
    elif route[2] == "z":
        first, second = route[0], route[1]
    else:
        first, second = route[0], route[2]
    bit = {"x": 1, "y": 2}
    off_first, off_second = bool(cls & bit[first]), bool(cls & bit[second])
    if route[0] == "z":
        if cls == 0:
            return ["z", first, second]
        return [second] if off_first and not off_second else []
    if route[2] == "z":
        ways = []
        if dist == 0 and cls == 0:
            ways = [first, second]
        elif dist == 0 and off_first and not off_second:
            ways = [second]
        return ways + ["z"]
    if off_second:
        return []
    return ([first] if dist == 0 and not off_first else []) + [second, "z"]


def sends_on(way, cc, pz):
    count = 0
    for piece in range(4 * cc, 4 * cc + 4):
        for cls in range(4):
            for src_z in range(4):
                ways = onward(ROUTES[piece], cls, abs(pz - src_z))
                if way in ("x", "y"):
                    count += way in ways
                elif way == "up":
                    count += "z" in ways and src_z <= pz < 3
                else:
                    count += "z" in ways and src_z >= pz > 0
    return count


def lanczos_kernel(
    vec_count,
    psi_ref, left_ref, op_hbm, right_ref,
    out_ref, alpha_ref, beta_ref,
    u_ref, stage_ref, env_l, env_r, kron_ref, x_ref, y_ref, sig_ref, part_ref, v_ref, w_ref, stat_ref, op_ref, turn_ref, flat_ref,
    recv_sem, send_sem, pair_send, pair_recv, part_sem, stat_sem, load_sem, out_sem, psi_sem,
):
    idx = lax.axis_index("rows")
    core = lax.rem(idx, 2)
    pos_x = lax.rem(idx // 2, 2)
    pos_y = lax.rem(idx // 4, 2)
    pos_z = idx // 8
    chip = idx // 2
    sib = idx + 1 - 2 * core
    next_x = idx + 2 - 4 * pos_x
    next_y = idx + 4 - 8 * pos_y

    def block(piece, first_row, rows):
        return u_ref.at[piece // 4, pl.ds(2 * (piece % 4), 2), pl.ds(pl.multiple_of(first_row, 16), rows), :]

    WAYS = {"x": 0, "y": 1, "up": 2, "down": 3}

    def copy(piece, src, way, first_row, rows):
        target = {"x": next_x, "y": next_y, "up": idx + 8, "down": idx - 8}[way]
        ref = block(piece, first_row, rows)
        return pltpu.make_async_remote_copy(
            src_ref=ref, dst_ref=ref, send_sem=send_sem.at[WAYS[way] + 4 * (piece // 4)],
            recv_sem=recv_sem.at[src, piece], device_id=(target,), device_id_type=MESH)

    def send(piece, src, way, first_row=None, rows=32):
        if first_row is None:
            first_row = 32 * src
        if way == "up":
            @pl.when(pos_z < 3)
            def _():
                copy(piece, src, way, first_row, rows).start()
        elif way == "down":
            @pl.when(pos_z > 0)
            def _():
                copy(piece, src, way, first_row, rows).start()
        else:
            copy(piece, src, way, first_row, rows).start()

    def send_own(piece, way, first_row=None, rows=32):
        for one in (("up", "down") if way == "z" else (way,)):
            send(piece, chip, one, first_row, rows)

    def arrival(piece, cls, dist):
        col_x = 1 - pos_x if cls & 1 else pos_x
        col_y = 1 - pos_y if cls & 2 else pos_y

        def act(src_z, heading):
            src = (src_z * 2 + col_y) * 2 + col_x
            copy(piece, src, "x", 32 * src, 32).wait_recv()
            for way in onward(ROUTES[piece], cls, dist):
                if way != "z":
                    send(piece, src, way)
                else:
                    for one in heading:
                        send(piece, src, one)

        if dist == 0:
            act(pos_z, ("up", "down"))
            return

        @pl.when(pos_z >= dist)
        def _():
            act(pos_z - dist, ("up",))

        @pl.when(pos_z + dist <= 3)
        def _():
            act(pos_z + dist, ("down",))

    def sends_done():
        def wait(count, way, cc):
            if count:
                ref = env_r.at[0, pl.ds(0, count), pl.ds(0, 32), :]
                pltpu.make_async_copy(ref, ref, send_sem.at[WAYS[way] + 4 * cc]).wait()

        for cc in range(2):
            wait(sends_on("x", cc, 0), "x", cc)
            wait(sends_on("y", cc, 0), "y", cc)
        for pz in range(4):
            @pl.when(pos_z == pz)
            def _():
                for cc in range(2):
                    wait(sends_on("up", cc, pz), "up", cc)
                    wait(sends_on("down", cc, pz), "down", cc)

    my_rows = pl.ds(pl.multiple_of(32 * chip + 16 * core, 16), 16)
    right_loads = [
        pltpu.make_async_copy(
            right_ref.at[:, pl.ds(pl.multiple_of(256 * core + 128 * cc, 128), 128), :], env_r.at[cc], load_sem.at[cc])
        for cc in range(2)]
    left_load = pltpu.make_async_copy(left_ref, env_l.at[:, core], load_sem.at[2])
    left_send = pltpu.make_async_remote_copy(
        src_ref=left_ref, dst_ref=env_l.at[:, core], send_sem=load_sem.at[3], recv_sem=load_sem.at[4],
        device_id=(sib,), device_id_type=MESH)
    left_send.start()
    left_load.start()
    psi_loads = [
        pltpu.make_async_copy(psi_ref.at[:, q // 4, q % 4, :], w_ref.at[pl.ds(16 * q, 16), :], psi_sem) for q in range(16)]
    for load in psi_loads:
        load.start()
    op_load = pltpu.make_async_copy(op_hbm, op_ref, load_sem.at[5])
    op_load.start()
    for load in right_loads:
        load.start()

    def build_kron():
        big_row = lax.broadcasted_iota(jnp.int32, (256, 256), 0)
        big_col = lax.broadcasted_iota(jnp.int32, (256, 256), 1)
        row_hi, row_lo = lax.shift_right_logical(big_row, 4), big_row & 15
        col_hi, col_lo = lax.shift_right_logical(big_col, 4), big_col & 15
        spread = jnp.where(row_lo == col_hi, 1.0, 0.0).astype(BF16)
        flat_ref[...] = jnp.transpose(op_ref[...].reshape(256, 32).astype(F32))

        def some(k8, carry):
            for kk in range(8):
                k = k8 * 8 + kk
                tall = jnp.where(row_hi == col_hi, flat_ref[pl.ds(k, 1), :], 0.0).astype(BF16)
                full = jnp.dot(tall, spread, preferred_element_type=F32)
                kron_ref[k] = jnp.where(row_lo == col_lo, full, 0.0).astype(BF16)
            return carry

        lax.fori_loop(0, 4, some, 0)

    def left_part(piece):
        for sub in range(2):
            rp = 2 * (piece % 4) + sub
            out = jnp.dot(env_l[...].reshape(1024, 512), u_ref[piece // 4, rp], preferred_element_type=F32)
            out = out.astype(BF16).reshape(32, 2, 16, 256)
            for ag in range(2):
                for par in range(2):
                    row = (2 * rp + par) * 16
                    x_ref[:, row:row + 16, ag * 128:(ag + 1) * 128] = out[:, ag, :, par * 128:(par + 1) * 128]

    def mid_part(part):
        for kk in range(8):
            k = 8 * (part % 4) + kk
            out = jnp.dot(kron_ref[k], x_ref[k], preferred_element_type=F32).astype(BF16)
            for ag in range(2):
                y_ref[ag, :, k * 128:(k + 1) * 128] = out[:, ag * 128:(ag + 1) * 128]

    def right_part(part):
        cc, who = part // 2, part % 2
        ag = 1 - core if who == 0 else core
        out = jnp.dot(y_ref[ag], env_r[cc].reshape(4096, 512), preferred_element_type=F32)
        sig_ref[who] = out if cc == 0 else sig_ref[who] + out

    lane = lax.broadcasted_iota(jnp.int32, (1, 128), 1)

    def total(val):
        cols = val.shape[1]
        part = val[:, 0:128]
        for first in range(128, cols, 128):
            part = part + val[:, first:first + 128]
        return jnp.sum(jnp.sum(part, axis=0, keepdims=True), axis=1, keepdims=True)

    def start_stats(dot_val, proj, sq_w, sq_v, cross):
        row = jnp.where(lane == 0, dot_val, 0.0)
        for which, val in ((1, proj), (2, sq_w), (3, sq_v), (4, cross)):
            row = jnp.where(lane == which, val, row)
        stat_ref[idx] = row

        def to_all(off, carry):
            pltpu.make_async_remote_copy(
                src_ref=stat_ref.at[idx], dst_ref=stat_ref.at[idx], send_sem=stat_sem.at[0], recv_sem=stat_sem.at[1],
                device_id=(lax.rem(idx + off, 32),), device_id_type=MESH).start()
            return carry

        lax.fori_loop(1, 32, to_all, 0)

    def finish_stats():
        others = stat_ref.at[pl.ds(0, 31)]
        pltpu.make_async_copy(others, others, stat_sem.at[1]).wait()
        pltpu.make_async_copy(others, others, stat_sem.at[0]).wait()

        def pick(row, which):
            return jnp.sum(jnp.where(lane == which, row, 0.0), axis=1, keepdims=True)

        rows = [stat_ref[d] for d in range(32)]
        whole = rows[0]
        for row in rows[1:]:
            whole = whole + row
        alpha = pick(whole, 0) / vec_count
        extra = jnp.zeros((1, 128), F32)
        for row in rows:
            delta = alpha - pltpu.roll(row, 2, 1)
            extra = extra + delta * (delta * row - 2.0 * pltpu.roll(row, 127, 1))
        beta_sq = jnp.sum(jnp.where(lane == 2, whole, jnp.where(lane == 3, extra, 0.0)), axis=1, keepdims=True)
        return alpha, jnp.sqrt(beta_sq / vec_count)

    def fold(val):
        return val[0:8] + val[8:16]

    def normalise(slot, prev, alpha, beta, proj, keep):
        delta = alpha - proj
        scale = 1.0 / beta
        acc = jnp.zeros((8, 512), F32)
        for q in range(16):
            rows = pl.ds(16 * q, 16)
            vec = (w_ref[rows, :] - delta * v_ref[prev, rows, :]) * scale
            v_ref[slot, rows, :] = vec
            acc = acc + fold(vec * vec)
            keep(q, vec)
        return acc

    def turn(slot):
        for q in range(16):
            turn_ref[:, q // 4, q % 4, :] = v_ref[slot, pl.ds(16 * q, 16), :]

    def out_copy(step):
        return pltpu.make_async_copy(turn_ref, out_ref.at[step], out_sem)

    for load in psi_loads:
        load.wait()
    acc = jnp.zeros((8, 512), F32)
    for q in range(16):
        rows = pl.ds(16 * q, 16)
        acc = acc + fold(w_ref[rows, :] * w_ref[rows, :])
        v_ref[1, rows, :] = jnp.zeros((16, 512), F32)
        v_ref[2, rows, :] = jnp.zeros((16, 512), F32)
    nought = jnp.zeros((1, 1), F32)
    start_stats(nought, nought, total(acc), nought, nought)
    op_load.wait()
    build_kron()

    def step_body(j, proj):
        cur = lax.rem(j, 3)
        prev = lax.rem(j + 2, 3)
        alpha, beta = finish_stats()

        def to_bf16(q, vec):
            low, high = vec[:, 0:256], vec[:, 256:512]
            own = jnp.where(core == 0, low, high).astype(BF16)
            far = jnp.where(core == 0, high, low).astype(BF16)
            lanes = slice(q % 2 * 128, q % 2 * 128 + 128)
            for cc in range(2):
                u_ref[cc, q // 2, my_rows, lanes] = own[:, cc * 128:(cc + 1) * 128]
                stage_ref[cc, q // 2, :, lanes] = far[:, cc * 128:(cc + 1) * 128]

        acc_v = normalise(cur, prev, alpha, beta, proj, to_bf16)

        def pair_copy(cc):
            return pltpu.make_async_remote_copy(
                src_ref=stage_ref.at[cc], dst_ref=u_ref.at[cc, :, my_rows, :],
                send_sem=pair_send.at[cc], recv_sem=pair_recv.at[cc], device_id=(sib,), device_id_type=MESH)

        for cc in range(2):
            pair_copy(cc).start()
        lead = 0
        while ORDER[lead][0] == "o":
            lead += 1
        for word in ORDER[:lead]:
            send_own(int(word[1]), word[2], 32 * chip + 16 * core, 16)
        for cc in range(2):
            pair_copy(cc).wait_recv()
            for word in ORDER[:lead]:
                if int(word[1]) // 4 == cc:
                    send_own(int(word[1]), word[2], 32 * chip + 16 * (1 - core), 16)
        sq_v = total(acc_v)

        @pl.when(j > 0)
        def _():
            alpha_ref[j - 1] = alpha[0, 0]
            beta_ref[j - 1] = beta[0, 0]
            out_copy(j - 1).wait()

        turn(cur)
        out_copy(j).start()

        part_copy = pltpu.make_async_remote_copy(
            src_ref=sig_ref.at[0], dst_ref=part_ref, send_sem=part_sem.at[0], recv_sem=part_sem.at[1],
            device_id=(sib,), device_id_type=MESH)
        loaded = False
        for word in ORDER[lead:]:
            what, piece = word[0], int(word[1])
            if what == "o":
                send_own(piece, word[2])
            elif what == "e":
                arrival(piece, CLASSES.index(word[2]), int(word[3]))
            elif what == "l":
                if not loaded:
                    loaded = True

                    @pl.when(j == 0)
                    def _():
                        left_load.wait()
                        left_send.wait()
                        for load in right_loads:
                            load.wait()
                left_part(piece)
            elif what == "m":
                mid_part(piece)
            else:
                right_part(piece)
                if piece == 2:
                    part_copy.start()
        part_copy.wait()
        for cc in range(2):
            pair_copy(cc).wait_send()
        sends_done()

        acc_p = jnp.zeros((8, 512), F32)
        for q in range(16):
            rows = pl.ds(16 * q, 16)
            sig = sig_ref[1, rows, :] + part_ref[rows, :]
            w_ref[rows, :] = sig
            acc_p = acc_p + fold(sig * v_ref[cur, rows, :])
        dot_val = total(acc_p)
        new_proj = jnp.where(sq_v > 0.0, dot_val / jnp.where(sq_v > 0.0, sq_v, 1.0), 0.0)
        beta_use = jnp.where(j > 0, beta, 0.0)
        acc_w = jnp.zeros((8, 512), F32)
        acc_c = jnp.zeros((8, 512), F32)
        for q in range(16):
            rows = pl.ds(16 * q, 16)
            vec = v_ref[cur, rows, :]
            res = w_ref[rows, :] - beta_use * v_ref[prev, rows, :] - new_proj * vec
            w_ref[rows, :] = res
            acc_w = acc_w + fold(res * res)
            acc_c = acc_c + fold(res * vec)
        start_stats(dot_val, new_proj, total(acc_w), sq_v, total(acc_c))
        return new_proj

    proj = lax.fori_loop(0, NUM_STEPS, step_body, nought)
    alpha, beta = finish_stats()
    last = NUM_STEPS % 3
    normalise(last, (NUM_STEPS - 1) % 3, alpha, beta, proj, lambda q, vec: None)
    out_copy(NUM_STEPS - 1).wait()
    turn(last)
    out_copy(NUM_STEPS).start()
    alpha_ref[NUM_STEPS - 1] = alpha[0, 0]
    beta_ref[NUM_STEPS - 1] = beta[0, 0]
    out_copy(NUM_STEPS).wait()


def solution(mesh):
    def local_run(wave_rows, left_rows, op_pair, right_env):
        rows, phys, _, bond = wave_rows.shape
        pair = phys * phys
        vec_count = float(bond * bond * pair)
        op_last = jnp.transpose(op_pair, (1, 2, 0))
        vecs, alpha, beta = pl.pallas_call(
            functools.partial(lanczos_kernel, vec_count),
            out_shape=(
                jax.ShapeDtypeStruct((NUM_STEPS + 1, rows, phys, phys, bond), F32),
                jax.ShapeDtypeStruct((NUM_STEPS,), F32),
                jax.ShapeDtypeStruct((NUM_STEPS,), F32),
            ),
            in_specs=[pl.BlockSpec(memory_space=pl.ANY)] * 4,
            out_specs=(
                pl.BlockSpec(memory_space=pl.ANY),
                pl.BlockSpec(memory_space=pltpu.SMEM),
                pl.BlockSpec(memory_space=pltpu.SMEM),
            ),
            scratch_shapes=[
                pltpu.VMEM((2, 8, 512, 256), BF16),
                pltpu.VMEM((2, 8, 16, 256), BF16),
                pltpu.VMEM((32, 2, 16, 512), BF16),
                pltpu.VMEM((2, 32, 128, 512), BF16),
                pltpu.VMEM((32, 256, 256), BF16),
                pltpu.VMEM((32, 256, 256), BF16),
                pltpu.VMEM((2, 256, 4096), BF16),
                pltpu.VMEM((2, 256, 512), F32),
                pltpu.VMEM((256, 512), F32),
                pltpu.VMEM((3, 256, 512), F32),
                pltpu.VMEM((256, 512), F32),
                pltpu.VMEM((32, 1, 128), F32),
                pltpu.VMEM((16, 16, 32), BF16),
                pltpu.VMEM((16, 4, 4, 512), F32),
                pltpu.VMEM((32, 256), F32),
                pltpu.SemaphoreType.DMA((16, 8)),
                pltpu.SemaphoreType.DMA((8,)),
                pltpu.SemaphoreType.DMA((2,)),
                pltpu.SemaphoreType.DMA((2,)),
                pltpu.SemaphoreType.DMA((2,)),
                pltpu.SemaphoreType.DMA((2,)),
                pltpu.SemaphoreType.DMA((6,)),
                pltpu.SemaphoreType.DMA,
                pltpu.SemaphoreType.DMA,
            ],
            compiler_params=pltpu.CompilerParams(has_side_effects=True, vmem_limit_bytes=60 * 1024 * 1024),
        )(wave_rows, left_rows, op_last, right_env)
        return vecs, alpha, beta

    return jax.shard_map(
        local_run, mesh=mesh,
        in_specs=(P("rows"), P(None, "rows"), P(), P()),
        out_specs=(P(None, "rows"), P(), P()), check_vma=False)
```

```python
import functools

import jax
import jax.numpy as jnp
from jax import lax
from jax.experimental import pallas as pl
from jax.experimental.pallas import tpu as pltpu
from jax.sharding import PartitionSpec as P

NUM_STEPS = 6
MESH = pl.DeviceIdType.MESH
F32 = jnp.float32
BF16 = jnp.bfloat16

ROUTES = ("zyx", "xzy", "zxy", "zyx", "zyx", "xzy", "zyx", "yxz")
ORDER = (
    "o2z", "o6x", "o2x", "o3y", "o4x", "o5x", "o4z", "o3z", "o2y", "o0z", "o6y", "o0y", "o1x", "o0x", "o1z", "o4y",
    "o1y", "o7x", "o3x", "o5z", "o7y", "o6z", "e2n1", "e3n1", "e2x0", "e0n1", "e6x0", "e1x0", "e7y0", "e0x0", "e2n2",
    "e3n2", "e0n2", "o7z", "e1x1", "e3y1", "e2x1", "e2d0", "e7x0", "e2y0", "e4n1", "e1n1", "e4y0", "e2x2", "e3n3",
    "e7d0", "e0n3", "e2n3", "e1x2", "e3y2", "e3y0", "e0y0", "e0y1", "e0x2", "e2x3", "e3x3", "e3y3", "e4n2", "e1x3",
    "e1d0", "e1n2", "e3x0", "e4n3", "e5x0", "e0y2", "e1n3", "e0y3", "e2y2", "e4x0", "e6n1", "e3x1", "e2y1", "e3d3",
    "e7y1", "e0x3", "e3d2", "e2d3", "e7n1", "e6n2", "e5n1", "e1y1", "e2d2", "e1d1", "e4y3", "e3d0", "e7d1", "e6n3",
    "e2d1", "e3d1", "e0x1", "e1d3", "e0d1", "e5x1", "e7x1", "e2y3", "e4x3", "l2", "e1y0", "e4y2", "e4x2", "e0d3",
    "e3x2", "e4y1", "e0d0", "l3", "e0d2", "e5n2", "l0", "e7d2", "e1y2", "e1d2", "e6y0", "e1y3", "l1", "e4x1", "e5x2",
    "e7y2", "m0", "m1", "e6y2", "e6y1", "e6x2", "e7n2", "m2", "m3", "e7x2", "e5n3", "o5y", "e4d2", "e6y3", "e4d3",
    "r0", "e5x3", "e4d0", "e7d3", "r1", "e6x3", "e5d1", "e4d1", "l4", "e7n3", "e5y3", "e6d2", "e7x3", "e5d0", "e6d0",
    "e6x1", "e7y3", "l7", "e6d3", "e6d1", "l6", "e5d3", "e5y0", "e5y1", "e5y2", "e5d2", "l5", "m4", "m5", "m6", "m7",
    "r2", "r3",
)


CLASSES = "nxyd"


def onward(route, cls, dist):
    if route[0] == "z":
        first, second = route[1], route[2]
    elif route[2] == "z":
        first, second = route[0], route[1]
    else:
        first, second = route[0], route[2]
    bit = {"x": 1, "y": 2}
    off_first, off_second = bool(cls & bit[first]), bool(cls & bit[second])
    if route[0] == "z":
        if cls == 0:
            return ["z", first, second]
        return [second] if off_first and not off_second else []
    if route[2] == "z":
        ways = []
        if dist == 0 and cls == 0:
            ways = [first, second]
        elif dist == 0 and off_first and not off_second:
            ways = [second]
        return ways + ["z"]
    if off_second:
        return []
    return ([first] if dist == 0 and not off_first else []) + [second, "z"]


def sends_on(way, cc, pz):
    count = 0
    for piece in range(4 * cc, 4 * cc + 4):
        for cls in range(4):
            for src_z in range(4):
                ways = onward(ROUTES[piece], cls, abs(pz - src_z))
                if way in ("x", "y"):
                    count += way in ways
                elif way == "up":
                    count += "z" in ways and src_z <= pz < 3
                else:
                    count += "z" in ways and src_z >= pz > 0
    return count


def lanczos_kernel(
    vec_count,
    psi_ref, left_ref, op_hbm, right_ref,
    out_ref, alpha_ref, beta_ref,
    u_ref, stage_ref, env_l, env_r, kron_ref, x_ref, y_ref, sig_ref, part_ref, v_ref, w_ref, stat_ref, op_ref, turn_ref, flat_ref,
    recv_sem, send_sem, pair_send, pair_recv, part_sem, stat_sem, load_sem, out_sem, psi_sem,
):
    idx = lax.axis_index("rows")
    core = lax.rem(idx, 2)
    pos_x = lax.rem(idx // 2, 2)
    pos_y = lax.rem(idx // 4, 2)
    pos_z = idx // 8
    chip = idx // 2
    sib = idx + 1 - 2 * core
    next_x = idx + 2 - 4 * pos_x
    next_y = idx + 4 - 8 * pos_y

    def block(piece, first_row, rows):
        return u_ref.at[piece // 4, pl.ds(2 * (piece % 4), 2), pl.ds(pl.multiple_of(first_row, 16), rows), :]

    WAYS = {"x": 0, "y": 1, "up": 2, "down": 3}

    def copy(piece, src, way, first_row, rows):
        target = {"x": next_x, "y": next_y, "up": idx + 8, "down": idx - 8}[way]
        ref = block(piece, first_row, rows)
        return pltpu.make_async_remote_copy(
            src_ref=ref, dst_ref=ref, send_sem=send_sem.at[WAYS[way] + 4 * (piece // 4)],
            recv_sem=recv_sem.at[src, piece], device_id=(target,), device_id_type=MESH)

    def send(piece, src, way, first_row=None, rows=32):
        if first_row is None:
            first_row = 32 * src
        if way == "up":
            @pl.when(pos_z < 3)
            def _():
                copy(piece, src, way, first_row, rows).start()
        elif way == "down":
            @pl.when(pos_z > 0)
            def _():
                copy(piece, src, way, first_row, rows).start()
        else:
            copy(piece, src, way, first_row, rows).start()

    def send_own(piece, way, first_row=None, rows=32):
        for one in (("up", "down") if way == "z" else (way,)):
            send(piece, chip, one, first_row, rows)

    def arrival(piece, cls, dist):
        col_x = 1 - pos_x if cls & 1 else pos_x
        col_y = 1 - pos_y if cls & 2 else pos_y

        def act(src_z, heading):
            src = (src_z * 2 + col_y) * 2 + col_x
            copy(piece, src, "x", 32 * src, 32).wait_recv()
            for way in onward(ROUTES[piece], cls, dist):
                if way != "z":
                    send(piece, src, way)
                else:
                    for one in heading:
                        send(piece, src, one)

        if dist == 0:
            act(pos_z, ("up", "down"))
            return

        @pl.when(pos_z >= dist)
        def _():
            act(pos_z - dist, ("up",))

        @pl.when(pos_z + dist <= 3)
        def _():
            act(pos_z + dist, ("down",))

    def sends_done():
        def wait(count, way, cc):
            if count:
                ref = env_r.at[0, pl.ds(0, count), pl.ds(0, 32), :]
                pltpu.make_async_copy(ref, ref, send_sem.at[WAYS[way] + 4 * cc]).wait()

        for cc in range(2):
            wait(sends_on("x", cc, 0), "x", cc)
            wait(sends_on("y", cc, 0), "y", cc)
        for pz in range(4):
            @pl.when(pos_z == pz)
            def _():
                for cc in range(2):
                    wait(sends_on("up", cc, pz), "up", cc)
                    wait(sends_on("down", cc, pz), "down", cc)

    my_rows = pl.ds(pl.multiple_of(32 * chip + 16 * core, 16), 16)
    right_loads = [
        pltpu.make_async_copy(
            right_ref.at[:, pl.ds(pl.multiple_of(256 * core + 128 * cc, 128), 128), :], env_r.at[cc], load_sem.at[cc])
        for cc in range(2)]
    left_load = pltpu.make_async_copy(left_ref, env_l.at[:, core], load_sem.at[2])
    left_send = pltpu.make_async_remote_copy(
        src_ref=left_ref, dst_ref=env_l.at[:, core], send_sem=load_sem.at[3], recv_sem=load_sem.at[4],
        device_id=(sib,), device_id_type=MESH)
    left_send.start()
    left_load.start()
    psi_loads = [
        pltpu.make_async_copy(psi_ref.at[:, q // 4, q % 4, :], w_ref.at[pl.ds(16 * q, 16), :], psi_sem) for q in range(16)]
    for load in psi_loads:
        load.start()
    op_load = pltpu.make_async_copy(op_hbm, op_ref, load_sem.at[5])
    op_load.start()
    for load in right_loads:
        load.start()

    def build_kron():
        big_row = lax.broadcasted_iota(jnp.int32, (256, 256), 0)
        big_col = lax.broadcasted_iota(jnp.int32, (256, 256), 1)
        row_hi, row_lo = lax.shift_right_logical(big_row, 4), big_row & 15
        col_hi, col_lo = lax.shift_right_logical(big_col, 4), big_col & 15
        spread = jnp.where(row_lo == col_hi, 1.0, 0.0).astype(BF16)
        flat_ref[...] = jnp.transpose(op_ref[...].reshape(256, 32).astype(F32))

        def some(k8, carry):
            for kk in range(8):
                k = k8 * 8 + kk
                tall = jnp.where(row_hi == col_hi, flat_ref[pl.ds(k, 1), :], 0.0).astype(BF16)
                full = jnp.dot(tall, spread, preferred_element_type=F32)
                kron_ref[k] = jnp.where(row_lo == col_lo, full, 0.0).astype(BF16)
            return carry

        lax.fori_loop(0, 4, some, 0)

    def left_part(piece):
        for sub in range(2):
            rp = 2 * (piece % 4) + sub
            out = jnp.dot(env_l[...].reshape(1024, 512), u_ref[piece // 4, rp], preferred_element_type=F32)
            out = out.astype(BF16).reshape(32, 2, 16, 256)
            for ag in range(2):
                for par in range(2):
                    row = (2 * rp + par) * 16
                    x_ref[:, row:row + 16, ag * 128:(ag + 1) * 128] = out[:, ag, :, par * 128:(par + 1) * 128]

    def mid_part(part):
        for kk in range(8):
            k = 8 * (part % 4) + kk
            out = jnp.dot(kron_ref[k], x_ref[k], preferred_element_type=F32).astype(BF16)
            for ag in range(2):
                y_ref[ag, :, k * 128:(k + 1) * 128] = out[:, ag * 128:(ag + 1) * 128]

    def right_part(part):
        cc, who = part // 2, part % 2
        ag = 1 - core if who == 0 else core
        out = jnp.dot(y_ref[ag], env_r[cc].reshape(4096, 512), preferred_element_type=F32)
        sig_ref[who] = out if cc == 0 else sig_ref[who] + out

    def right_half(half):
        lanes = slice(256 * half, 256 * half + 256)
        rhs = env_r[1, :, :, lanes].reshape(4096, 256)
        sig_ref[0, :, lanes] = sig_ref[0, :, lanes] + jnp.dot(y_ref[1 - core], rhs, preferred_element_type=F32)

    lane = lax.broadcasted_iota(jnp.int32, (1, 128), 1)

    def total(val):
        cols = val.shape[1]
        part = val[:, 0:128]
        for first in range(128, cols, 128):
            part = part + val[:, first:first + 128]
        return jnp.sum(jnp.sum(part, axis=0, keepdims=True), axis=1, keepdims=True)

    def start_stats(dot_val, proj, sq_w, sq_v, cross):
        row = jnp.where(lane == 0, dot_val, 0.0)
        for which, val in ((1, proj), (2, sq_w), (3, sq_v), (4, cross)):
            row = jnp.where(lane == which, val, row)
        stat_ref[idx] = row

        flips = [(1 - pos_x if m & 2 else pos_x) * 2 + (1 - core if m & 1 else core) for m in range(4)]
        flips += [flip + 4 * (1 - pos_y) for flip in flips[:4]]
        flips = [flip + 4 * pos_y for flip in flips[:4]] + flips[4:]
        z_low, z_high = lax.rem(pos_z, 2), pos_z // 2
        for m in range(31, 0, -1):
            high = 1 - z_high if m & 16 else z_high
            low = 1 - z_low if m & 8 else z_low
            pltpu.make_async_remote_copy(
                src_ref=stat_ref.at[idx], dst_ref=stat_ref.at[idx], send_sem=stat_sem.at[0], recv_sem=stat_sem.at[1],
                device_id=(16 * high + 8 * low + flips[m % 8],), device_id_type=MESH).start()

    def finish_stats():
        others = stat_ref.at[pl.ds(0, 31)]
        pltpu.make_async_copy(others, others, stat_sem.at[1]).wait()
        pltpu.make_async_copy(others, others, stat_sem.at[0]).wait()

        def pick(row, which):
            return jnp.sum(jnp.where(lane == which, row, 0.0), axis=1, keepdims=True)

        rows = [stat_ref[d] for d in range(32)]
        whole = rows[0]
        for row in rows[1:]:
            whole = whole + row
        alpha = pick(whole, 0) / vec_count
        extra = jnp.zeros((1, 128), F32)
        for row in rows:
            delta = alpha - pltpu.roll(row, 2, 1)
            extra = extra + delta * (delta * row - 2.0 * pltpu.roll(row, 127, 1))
        beta_sq = jnp.sum(jnp.where(lane == 2, whole, jnp.where(lane == 3, extra, 0.0)), axis=1, keepdims=True)
        return alpha, jnp.sqrt(beta_sq / vec_count)

    def fold(val):
        return val[0:8] + val[8:16]

    def normalise(slot, prev, alpha, beta, proj, keep):
        delta = alpha - proj
        scale = 1.0 / beta
        acc = jnp.zeros((8, 512), F32)
        for q in range(16):
            rows = pl.ds(16 * q, 16)
            vec = (w_ref[rows, :] - delta * v_ref[prev, rows, :]) * scale
            v_ref[slot, rows, :] = vec
            acc = acc + fold(vec * vec)
            keep(q, vec)
        return acc

    def turn(slot):
        for q in range(16):
            turn_ref[:, q // 4, q % 4, :] = v_ref[slot, pl.ds(16 * q, 16), :]

    def out_copy(step):
        return pltpu.make_async_copy(turn_ref, out_ref.at[step], out_sem)

    for load in psi_loads:
        load.wait()
    acc = jnp.zeros((8, 512), F32)
    for q in range(16):
        rows = pl.ds(16 * q, 16)
        acc = acc + fold(w_ref[rows, :] * w_ref[rows, :])
        v_ref[1, rows, :] = jnp.zeros((16, 512), F32)
        v_ref[2, rows, :] = jnp.zeros((16, 512), F32)
    nought = jnp.zeros((1, 1), F32)
    start_stats(nought, nought, total(acc), nought, nought)
    op_load.wait()
    build_kron()

    def step_body(j, proj):
        cur = lax.rem(j, 3)
        prev = lax.rem(j + 2, 3)
        alpha, beta = finish_stats()

        def to_bf16(q, vec):
            low, high = vec[:, 0:256], vec[:, 256:512]
            own = jnp.where(core == 0, low, high).astype(BF16)
            far = jnp.where(core == 0, high, low).astype(BF16)
            lanes = slice(q % 2 * 128, q % 2 * 128 + 128)
            for cc in range(2):
                u_ref[cc, q // 2, my_rows, lanes] = own[:, cc * 128:(cc + 1) * 128]
                stage_ref[cc, q // 2, :, lanes] = far[:, cc * 128:(cc + 1) * 128]

        acc_v = normalise(cur, prev, alpha, beta, proj, to_bf16)

        def pair_copy(cc):
            return pltpu.make_async_remote_copy(
                src_ref=stage_ref.at[cc], dst_ref=u_ref.at[cc, :, my_rows, :],
                send_sem=pair_send.at[cc], recv_sem=pair_recv.at[cc], device_id=(sib,), device_id_type=MESH)

        for cc in range(2):
            pair_copy(cc).start()
        lead = 0
        while ORDER[lead][0] == "o":
            lead += 1
        for word in ORDER[:lead]:
            send_own(int(word[1]), word[2], 32 * chip + 16 * core, 16)
        sq_v = total(acc_v)

        @pl.when(j > 0)
        def _():
            alpha_ref[j - 1] = alpha[0, 0]
            beta_ref[j - 1] = beta[0, 0]
            out_copy(j - 1).wait()

        turn(cur)
        out_copy(j).start()
        for cc in range(2):
            pair_copy(cc).wait_recv()
            for word in ORDER[:lead]:
                if int(word[1]) // 4 == cc:
                    send_own(int(word[1]), word[2], 32 * chip + 16 * (1 - core), 16)

        def part_copy(half):
            lanes = slice(256 * half, 256 * half + 256)
            return pltpu.make_async_remote_copy(
                src_ref=sig_ref.at[0, :, lanes], dst_ref=part_ref.at[:, lanes],
                send_sem=part_sem.at[half], recv_sem=part_sem.at[2 + half], device_id=(sib,), device_id_type=MESH)

        loaded = False
        for word in ORDER[lead:]:
            what, piece = word[0], int(word[1])
            if what == "o":
                send_own(piece, word[2])
            elif what == "e":
                arrival(piece, CLASSES.index(word[2]), int(word[3]))
            elif what == "l":
                if not loaded:
                    loaded = True

                    @pl.when(j == 0)
                    def _():
                        left_load.wait()
                        left_send.wait()
                        for load in right_loads:
                            load.wait()
                left_part(piece)
            elif what == "m":
                mid_part(piece)
            else:
                right_part(piece)
                if piece == 2:
                    for half in range(2):
                        part_copy(half).start()
        for cc in range(2):
            pair_copy(cc).wait_send()
        sends_done()
        for half in range(2):
            part_copy(half).wait()
        acc_p = jnp.zeros((8, 512), F32)
        for q in range(16):
            rows = pl.ds(16 * q, 16)
            sig = sig_ref[1, rows, :] + part_ref[rows, :]
            w_ref[rows, :] = sig
            acc_p = acc_p + fold(sig * v_ref[cur, rows, :])
        dot_val = total(acc_p)
        new_proj = jnp.where(sq_v > 0.0, dot_val / jnp.where(sq_v > 0.0, sq_v, 1.0), 0.0)
        beta_use = jnp.where(j > 0, beta, 0.0)
        acc_w = jnp.zeros((8, 512), F32)
        acc_c = jnp.zeros((8, 512), F32)
        for q in range(16):
            rows = pl.ds(16 * q, 16)
            vec = v_ref[cur, rows, :]
            res = w_ref[rows, :] - beta_use * v_ref[prev, rows, :] - new_proj * vec
            w_ref[rows, :] = res
            acc_w = acc_w + fold(res * res)
            acc_c = acc_c + fold(res * vec)
        start_stats(dot_val, new_proj, total(acc_w), sq_v, total(acc_c))
        return new_proj

    proj = lax.fori_loop(0, NUM_STEPS, step_body, nought)
    alpha, beta = finish_stats()
    last = NUM_STEPS % 3
    normalise(last, (NUM_STEPS - 1) % 3, alpha, beta, proj, lambda q, vec: None)
    out_copy(NUM_STEPS - 1).wait()
    turn(last)
    out_copy(NUM_STEPS).start()
    alpha_ref[NUM_STEPS - 1] = alpha[0, 0]
    beta_ref[NUM_STEPS - 1] = beta[0, 0]
    out_copy(NUM_STEPS).wait()


def solution(mesh):
    def local_run(wave_rows, left_rows, op_pair, right_env):
        rows, phys, _, bond = wave_rows.shape
        pair = phys * phys
        vec_count = float(bond * bond * pair)
        op_last = jnp.transpose(op_pair, (1, 2, 0))
        vecs, alpha, beta = pl.pallas_call(
            functools.partial(lanczos_kernel, vec_count),
            out_shape=(
                jax.ShapeDtypeStruct((NUM_STEPS + 1, rows, phys, phys, bond), F32),
                jax.ShapeDtypeStruct((NUM_STEPS,), F32),
                jax.ShapeDtypeStruct((NUM_STEPS,), F32),
            ),
            in_specs=[pl.BlockSpec(memory_space=pl.ANY)] * 4,
            out_specs=(
                pl.BlockSpec(memory_space=pl.ANY),
                pl.BlockSpec(memory_space=pltpu.SMEM),
                pl.BlockSpec(memory_space=pltpu.SMEM),
            ),
            scratch_shapes=[
                pltpu.VMEM((2, 8, 512, 256), BF16),
                pltpu.VMEM((2, 8, 16, 256), BF16),
                pltpu.VMEM((32, 2, 16, 512), BF16),
                pltpu.VMEM((2, 32, 128, 512), BF16),
                pltpu.VMEM((32, 256, 256), BF16),
                pltpu.VMEM((32, 256, 256), BF16),
                pltpu.VMEM((2, 256, 4096), BF16),
                pltpu.VMEM((2, 256, 512), F32),
                pltpu.VMEM((256, 512), F32),
                pltpu.VMEM((3, 256, 512), F32),
                pltpu.VMEM((256, 512), F32),
                pltpu.VMEM((32, 1, 128), F32),
                pltpu.VMEM((16, 16, 32), BF16),
                pltpu.VMEM((16, 4, 4, 512), F32),
                pltpu.VMEM((32, 256), F32),
                pltpu.SemaphoreType.DMA((16, 8)),
                pltpu.SemaphoreType.DMA((8,)),
                pltpu.SemaphoreType.DMA((2,)),
                pltpu.SemaphoreType.DMA((2,)),
                pltpu.SemaphoreType.DMA((4,)),
                pltpu.SemaphoreType.DMA((2,)),
                pltpu.SemaphoreType.DMA((6,)),
                pltpu.SemaphoreType.DMA,
                pltpu.SemaphoreType.DMA,
            ],
            compiler_params=pltpu.CompilerParams(has_side_effects=True, vmem_limit_bytes=40 * 1024 * 1024),
        )(wave_rows, left_rows, op_last, right_env)
        return vecs, alpha, beta

    return jax.shard_map(
        local_run, mesh=mesh,
        in_specs=(P("rows"), P(None, "rows"), P(), P()),
        out_specs=(P(None, "rows"), P(), P()), check_vma=False)
```

```python
import functools

import jax
import jax.numpy as jnp
from jax import lax
from jax.experimental import pallas as pl
from jax.experimental.pallas import tpu as pltpu
from jax.sharding import PartitionSpec as P

NUM_STEPS = 6
MESH = pl.DeviceIdType.MESH
F32 = jnp.float32
BF16 = jnp.bfloat16

ROUTES = ("zyx", "zyx", "xzy", "zyx", "xzy", "zxy", "zyx", "yxz")
ORDER = (
    "o1z", "o7x", "o0y", "o7y", "o5x", "o0z", "o5y", "o3x", "o6z", "o1x", "o1y", "o3y", "o2x", "o4y", "o3z", "o2z",
    "o0x", "o5z", "o4x", "e1n1", "e0n1", "e7y0", "e3y0", "e3n1", "e4x0", "e1n2", "e0n2", "e0y0", "e2n1", "e3n2",
    "e1y0", "e6n1", "e2x0", "o6y", "e1n3", "e3n3", "o4z", "e0n3", "e1y1", "e1x0", "e5x0", "e1y2", "e2n2", "e3d0",
    "e1y3", "e7x0", "e2n3", "e2x1", "e7d0", "e3y2", "e0x3", "o7z", "e1x2", "e1x1", "e0y3", "e0y1", "e0y2", "o2y",
    "e1x3", "e3y3", "e0x1", "e2x2", "e0x0", "e3x0", "e1d0", "e3y1", "e6n2", "e4d0", "e5n1", "e2x3", "e4x1", "e1d3",
    "e2d0", "e6n3", "e5n2", "e4n1", "e6x1", "e3x1", "e7x1", "e3x3", "e1d1", "e4x2", "e1d2", "e0d0", "e3d3", "e5n3",
    "e2y3", "o6x", "e6y0", "e2y0", "e3x2", "l1", "e7y1", "e2y1", "e4n2", "e7n1", "e2d3", "e0d1", "e2y2", "e7d1",
    "e2d2", "e0d3", "e2d1", "e0x2", "e6y1", "e0d2", "l2", "e3d2", "e3d1", "l3", "e7x2", "l0", "e6y3", "m0", "e4x3",
    "e7y2", "e5y1", "e5y0", "m1", "m2", "e4n3", "e5x3", "e6y2", "e7n2", "e5x1", "m3", "e5x2", "r0", "e4d1", "e7d2",
    "e6x2", "e5y2", "e4y1", "r1", "e6x3", "e4y3", "e4d3", "e6d3", "e4y2", "e7y3", "e4d2", "e4y0", "l4", "e6d2",
    "e5d0", "e6x0", "e6d0", "e6d1", "l6", "e5y3", "e7n3", "e7d3", "e5d1", "e7x3", "l7", "e5d2", "e5d3", "l5", "m4",
    "m5", "m6", "m7", "r2", "r3",
)


CLASSES = "nxyd"


def onward(route, cls, dist):
    if route[0] == "z":
        first, second = route[1], route[2]
    elif route[2] == "z":
        first, second = route[0], route[1]
    else:
        first, second = route[0], route[2]
    bit = {"x": 1, "y": 2}
    off_first, off_second = bool(cls & bit[first]), bool(cls & bit[second])
    if route[0] == "z":
        if cls == 0:
            return ["z", first, second]
        return [second] if off_first and not off_second else []
    if route[2] == "z":
        ways = []
        if dist == 0 and cls == 0:
            ways = [first, second]
        elif dist == 0 and off_first and not off_second:
            ways = [second]
        return ways + ["z"]
    if off_second:
        return []
    return ([first] if dist == 0 and not off_first else []) + [second, "z"]


def sends_on(way, cc, pz):
    count = 0
    for piece in range(4 * cc, 4 * cc + 4):
        for cls in range(4):
            for src_z in range(4):
                ways = onward(ROUTES[piece], cls, abs(pz - src_z))
                if way in ("x", "y"):
                    count += way in ways
                elif way == "up":
                    count += "z" in ways and src_z <= pz < 3
                else:
                    count += "z" in ways and src_z >= pz > 0
    return count


def lanczos_kernel(
    vec_count,
    psi_ref, left_ref, op_hbm, right_ref,
    out_ref, alpha_ref, beta_ref,
    u_ref, stage_ref, env_l, env_r, kron_ref, x_ref, y_ref, sig_ref, part_ref, v_ref, w_ref, stat_ref, op_ref, turn_ref, flat_ref,
    recv_sem, send_sem, pair_send, pair_recv, part_sem, stat_sem, load_sem, out_sem, psi_sem,
):
    idx = lax.axis_index("rows")
    core = lax.rem(idx, 2)
    pos_x = lax.rem(idx // 2, 2)
    pos_y = lax.rem(idx // 4, 2)
    pos_z = idx // 8
    chip = idx // 2
    sib = idx + 1 - 2 * core
    next_x = idx + 2 - 4 * pos_x
    next_y = idx + 4 - 8 * pos_y

    def block(piece, first_row, rows):
        return u_ref.at[piece // 4, pl.ds(2 * (piece % 4), 2), pl.ds(pl.multiple_of(first_row, 16), rows), :]

    WAYS = {"x": 0, "y": 1, "up": 2, "down": 3}

    def copy(piece, src, way, first_row, rows):
        target = {"x": next_x, "y": next_y, "up": idx + 8, "down": idx - 8}[way]
        ref = block(piece, first_row, rows)
        return pltpu.make_async_remote_copy(
            src_ref=ref, dst_ref=ref, send_sem=send_sem.at[WAYS[way] + 4 * (piece // 4)],
            recv_sem=recv_sem.at[src, piece], device_id=(target,), device_id_type=MESH)

    def send(piece, src, way, first_row=None, rows=32):
        if first_row is None:
            first_row = 32 * src
        if way == "up":
            @pl.when(pos_z < 3)
            def _():
                copy(piece, src, way, first_row, rows).start()
        elif way == "down":
            @pl.when(pos_z > 0)
            def _():
                copy(piece, src, way, first_row, rows).start()
        else:
            copy(piece, src, way, first_row, rows).start()

    def send_own(piece, way, first_row=None, rows=32):
        for one in (("up", "down") if way == "z" else (way,)):
            send(piece, chip, one, first_row, rows)

    def arrival(piece, cls, dist):
        col_x = 1 - pos_x if cls & 1 else pos_x
        col_y = 1 - pos_y if cls & 2 else pos_y

        def act(src_z, heading):
            src = (src_z * 2 + col_y) * 2 + col_x
            copy(piece, src, "x", 32 * src, 32).wait_recv()
            for way in onward(ROUTES[piece], cls, dist):
                if way != "z":
                    send(piece, src, way)
                else:
                    for one in heading:
                        send(piece, src, one)

        if dist == 0:
            act(pos_z, ("up", "down"))
            return

        @pl.when(pos_z >= dist)
        def _():
            act(pos_z - dist, ("up",))

        @pl.when(pos_z + dist <= 3)
        def _():
            act(pos_z + dist, ("down",))

    def sends_done():
        def wait(count, way, cc):
            if count:
                ref = env_r.at[0, pl.ds(0, count), pl.ds(0, 32), :]
                pltpu.make_async_copy(ref, ref, send_sem.at[WAYS[way] + 4 * cc]).wait()

        for cc in range(2):
            wait(sends_on("x", cc, 0), "x", cc)
            wait(sends_on("y", cc, 0), "y", cc)
        for pz in range(4):
            @pl.when(pos_z == pz)
            def _():
                for cc in range(2):
                    wait(sends_on("up", cc, pz), "up", cc)
                    wait(sends_on("down", cc, pz), "down", cc)

    my_rows = pl.ds(pl.multiple_of(32 * chip + 16 * core, 16), 16)
    right_loads = [
        pltpu.make_async_copy(
            right_ref.at[:, pl.ds(pl.multiple_of(256 * core + 128 * cc, 128), 128), :], env_r.at[cc], load_sem.at[cc])
        for cc in range(2)]
    left_load = pltpu.make_async_copy(left_ref, env_l.at[:, core], load_sem.at[2])
    left_send = pltpu.make_async_remote_copy(
        src_ref=left_ref, dst_ref=env_l.at[:, core], send_sem=load_sem.at[3], recv_sem=load_sem.at[4],
        device_id=(sib,), device_id_type=MESH)
    left_send.start()
    left_load.start()
    psi_loads = [
        pltpu.make_async_copy(psi_ref.at[:, q // 4, q % 4, :], w_ref.at[pl.ds(16 * q, 16), :], psi_sem) for q in range(16)]
    for load in psi_loads:
        load.start()
    op_load = pltpu.make_async_copy(op_hbm, op_ref, load_sem.at[5])
    op_load.start()
    for load in right_loads:
        load.start()

    def build_kron():
        big_row = lax.broadcasted_iota(jnp.int32, (256, 256), 0)
        big_col = lax.broadcasted_iota(jnp.int32, (256, 256), 1)
        row_hi, row_lo = lax.shift_right_logical(big_row, 4), big_row & 15
        col_hi, col_lo = lax.shift_right_logical(big_col, 4), big_col & 15
        spread = jnp.where(row_lo == col_hi, 1.0, 0.0).astype(BF16)
        flat_ref[...] = jnp.transpose(op_ref[...].reshape(256, 32).astype(F32))

        def some(k8, carry):
            for kk in range(8):
                k = k8 * 8 + kk
                tall = jnp.where(row_hi == col_hi, flat_ref[pl.ds(k, 1), :], 0.0).astype(BF16)
                full = jnp.dot(tall, spread, preferred_element_type=F32)
                kron_ref[k] = jnp.where(row_lo == col_lo, full, 0.0).astype(BF16)
            return carry

        lax.fori_loop(0, 4, some, 0)

    def left_part(piece):
        for sub in range(2):
            rp = 2 * (piece % 4) + sub
            out = jnp.dot(env_l[...].reshape(1024, 512), u_ref[piece // 4, rp], preferred_element_type=F32)
            out = out.astype(BF16).reshape(32, 2, 16, 256)
            for ag in range(2):
                for par in range(2):
                    row = (2 * rp + par) * 16
                    x_ref[:, row:row + 16, ag * 128:(ag + 1) * 128] = out[:, ag, :, par * 128:(par + 1) * 128]

    def mid_part(part):
        for kk in range(8):
            k = 8 * (part % 4) + kk
            out = jnp.dot(kron_ref[k], x_ref[k], preferred_element_type=F32).astype(BF16)
            for ag in range(2):
                y_ref[ag, :, k * 128:(k + 1) * 128] = out[:, ag * 128:(ag + 1) * 128]

    def right_part(part):
        cc, who = part // 2, part % 2
        ag = 1 - core if who == 0 else core
        out = jnp.dot(y_ref[ag], env_r[cc].reshape(4096, 512), preferred_element_type=F32)
        sig_ref[who] = out if cc == 0 else sig_ref[who] + out

    def right_half(half):
        lanes = slice(256 * half, 256 * half + 256)
        rhs = env_r[1, :, :, lanes].reshape(4096, 256)
        sig_ref[0, :, lanes] = sig_ref[0, :, lanes] + jnp.dot(y_ref[1 - core], rhs, preferred_element_type=F32)

    lane = lax.broadcasted_iota(jnp.int32, (1, 128), 1)

    def total(val):
        cols = val.shape[1]
        part = val[:, 0:128]
        for first in range(128, cols, 128):
            part = part + val[:, first:first + 128]
        return jnp.sum(jnp.sum(part, axis=0, keepdims=True), axis=1, keepdims=True)

    def start_stats(dot_val, proj, sq_w, sq_v, cross):
        row = jnp.where(lane == 0, dot_val, 0.0)
        for which, val in ((1, proj), (2, sq_w), (3, sq_v), (4, cross)):
            row = jnp.where(lane == which, val, row)
        stat_ref[idx] = row

        flips = [(1 - pos_x if m & 2 else pos_x) * 2 + (1 - core if m & 1 else core) for m in range(4)]
        flips += [flip + 4 * (1 - pos_y) for flip in flips[:4]]
        flips = [flip + 4 * pos_y for flip in flips[:4]] + flips[4:]
        z_low, z_high = lax.rem(pos_z, 2), pos_z // 2
        for m in range(31, 0, -1):
            high = 1 - z_high if m & 16 else z_high
            low = 1 - z_low if m & 8 else z_low
            pltpu.make_async_remote_copy(
                src_ref=stat_ref.at[idx], dst_ref=stat_ref.at[idx], send_sem=stat_sem.at[0], recv_sem=stat_sem.at[1],
                device_id=(16 * high + 8 * low + flips[m % 8],), device_id_type=MESH).start()

    def finish_stats():
        others = stat_ref.at[pl.ds(0, 31)]
        pltpu.make_async_copy(others, others, stat_sem.at[1]).wait()
        pltpu.make_async_copy(others, others, stat_sem.at[0]).wait()

        def pick(row, which):
            return jnp.sum(jnp.where(lane == which, row, 0.0), axis=1, keepdims=True)

        rows = [stat_ref[d] for d in range(32)]
        whole = rows[0]
        for row in rows[1:]:
            whole = whole + row
        alpha = pick(whole, 0) / vec_count
        extra = jnp.zeros((1, 128), F32)
        for row in rows:
            delta = alpha - pltpu.roll(row, 2, 1)
            extra = extra + delta * (delta * row - 2.0 * pltpu.roll(row, 127, 1))
        beta_sq = jnp.sum(jnp.where(lane == 2, whole, jnp.where(lane == 3, extra, 0.0)), axis=1, keepdims=True)
        return alpha, jnp.sqrt(beta_sq / vec_count)

    def fold(val):
        return val[0:8] + val[8:16]

    def normalise(slot, prev, alpha, beta, proj, keep):
        delta = alpha - proj
        scale = 1.0 / beta
        acc = jnp.zeros((8, 512), F32)
        for q in range(16):
            rows = pl.ds(16 * q, 16)
            vec = (w_ref[rows, :] - delta * v_ref[prev, rows, :]) * scale
            v_ref[slot, rows, :] = vec
            acc = acc + fold(vec * vec)
            keep(q, vec)
        return acc

    def turn(slot):
        for q in range(16):
            turn_ref[:, q // 4, q % 4, :] = v_ref[slot, pl.ds(16 * q, 16), :]

    def out_copy(step):
        return pltpu.make_async_copy(turn_ref, out_ref.at[step], out_sem)

    for load in psi_loads:
        load.wait()
    acc = jnp.zeros((8, 512), F32)
    for q in range(16):
        rows = pl.ds(16 * q, 16)
        acc = acc + fold(w_ref[rows, :] * w_ref[rows, :])
        v_ref[1, rows, :] = jnp.zeros((16, 512), F32)
        v_ref[2, rows, :] = jnp.zeros((16, 512), F32)
    nought = jnp.zeros((1, 1), F32)
    start_stats(nought, nought, total(acc), nought, nought)
    op_load.wait()
    build_kron()

    def step_body(j, proj):
        cur = lax.rem(j, 3)
        prev = lax.rem(j + 2, 3)
        alpha, beta = finish_stats()

        def to_bf16(q, vec):
            low, high = vec[:, 0:256], vec[:, 256:512]
            own = jnp.where(core == 0, low, high).astype(BF16)
            far = jnp.where(core == 0, high, low).astype(BF16)
            lanes = slice(q % 2 * 128, q % 2 * 128 + 128)
            for cc in range(2):
                u_ref[cc, q // 2, my_rows, lanes] = own[:, cc * 128:(cc + 1) * 128]
                stage_ref[cc, q // 2, :, lanes] = far[:, cc * 128:(cc + 1) * 128]

        acc_v = normalise(cur, prev, alpha, beta, proj, to_bf16)

        def pair_copy(cc):
            return pltpu.make_async_remote_copy(
                src_ref=stage_ref.at[cc], dst_ref=u_ref.at[cc, :, my_rows, :],
                send_sem=pair_send.at[cc], recv_sem=pair_recv.at[cc], device_id=(sib,), device_id_type=MESH)

        for cc in range(2):
            pair_copy(cc).start()
        lead = 0
        while ORDER[lead][0] == "o":
            lead += 1
        for word in ORDER[:lead]:
            send_own(int(word[1]), word[2], 32 * chip + 16 * core, 16)
        sq_v = total(acc_v)

        @pl.when(j > 0)
        def _():
            alpha_ref[j - 1] = alpha[0, 0]
            beta_ref[j - 1] = beta[0, 0]
            out_copy(j - 1).wait()

        turn(cur)
        out_copy(j).start()
        for cc in range(2):
            pair_copy(cc).wait_recv()
            for word in ORDER[:lead]:
                if int(word[1]) // 4 == cc:
                    send_own(int(word[1]), word[2], 32 * chip + 16 * (1 - core), 16)

        def part_copy(half):
            lanes = slice(256 * half, 256 * half + 256)
            return pltpu.make_async_remote_copy(
                src_ref=sig_ref.at[0, :, lanes], dst_ref=part_ref.at[:, lanes],
                send_sem=part_sem.at[half], recv_sem=part_sem.at[2 + half], device_id=(sib,), device_id_type=MESH)

        loaded = False
        for word in ORDER[lead:]:
            what, piece = word[0], int(word[1])
            if what == "o":
                send_own(piece, word[2])
            elif what == "e":
                arrival(piece, CLASSES.index(word[2]), int(word[3]))
            elif what == "l":
                if not loaded:
                    loaded = True

                    @pl.when(j == 0)
                    def _():
                        left_load.wait()
                        left_send.wait()
                        for load in right_loads:
                            load.wait()
                left_part(piece)
            elif what == "m":
                mid_part(piece)
            else:
                right_part(piece)
                if piece == 2:
                    for half in range(2):
                        part_copy(half).start()
        for cc in range(2):
            pair_copy(cc).wait_send()
        sends_done()
        for half in range(2):
            part_copy(half).wait()
        acc_p = jnp.zeros((8, 512), F32)
        for q in range(16):
            rows = pl.ds(16 * q, 16)
            sig = sig_ref[1, rows, :] + part_ref[rows, :]
            w_ref[rows, :] = sig
            acc_p = acc_p + fold(sig * v_ref[cur, rows, :])
        dot_val = total(acc_p)
        new_proj = jnp.where(sq_v > 0.0, dot_val / jnp.where(sq_v > 0.0, sq_v, 1.0), 0.0)
        beta_use = jnp.where(j > 0, beta, 0.0)
        acc_w = jnp.zeros((8, 512), F32)
        acc_c = jnp.zeros((8, 512), F32)
        for q in range(16):
            rows = pl.ds(16 * q, 16)
            vec = v_ref[cur, rows, :]
            res = w_ref[rows, :] - beta_use * v_ref[prev, rows, :] - new_proj * vec
            w_ref[rows, :] = res
            acc_w = acc_w + fold(res * res)
            acc_c = acc_c + fold(res * vec)
        start_stats(dot_val, new_proj, total(acc_w), sq_v, total(acc_c))
        return new_proj

    proj = lax.fori_loop(0, NUM_STEPS, step_body, nought)
    alpha, beta = finish_stats()
    last = NUM_STEPS % 3
    normalise(last, (NUM_STEPS - 1) % 3, alpha, beta, proj, lambda q, vec: None)
    out_copy(NUM_STEPS - 1).wait()
    turn(last)
    out_copy(NUM_STEPS).start()
    alpha_ref[NUM_STEPS - 1] = alpha[0, 0]
    beta_ref[NUM_STEPS - 1] = beta[0, 0]
    out_copy(NUM_STEPS).wait()


def solution(mesh):
    def local_run(wave_rows, left_rows, op_pair, right_env):
        rows, phys, _, bond = wave_rows.shape
        pair = phys * phys
        vec_count = float(bond * bond * pair)
        op_last = jnp.transpose(op_pair, (1, 2, 0))
        vecs, alpha, beta = pl.pallas_call(
            functools.partial(lanczos_kernel, vec_count),
            out_shape=(
                jax.ShapeDtypeStruct((NUM_STEPS + 1, rows, phys, phys, bond), F32),
                jax.ShapeDtypeStruct((NUM_STEPS,), F32),
                jax.ShapeDtypeStruct((NUM_STEPS,), F32),
            ),
            in_specs=[pl.BlockSpec(memory_space=pl.ANY)] * 4,
            out_specs=(
                pl.BlockSpec(memory_space=pl.ANY),
                pl.BlockSpec(memory_space=pltpu.SMEM),
                pl.BlockSpec(memory_space=pltpu.SMEM),
            ),
            scratch_shapes=[
                pltpu.VMEM((2, 8, 512, 256), BF16),
                pltpu.VMEM((2, 8, 16, 256), BF16),
                pltpu.VMEM((32, 2, 16, 512), BF16),
                pltpu.VMEM((2, 32, 128, 512), BF16),
                pltpu.VMEM((32, 256, 256), BF16),
                pltpu.VMEM((32, 256, 256), BF16),
                pltpu.VMEM((2, 256, 4096), BF16),
                pltpu.VMEM((2, 256, 512), F32),
                pltpu.VMEM((256, 512), F32),
                pltpu.VMEM((3, 256, 512), F32),
                pltpu.VMEM((256, 512), F32),
                pltpu.VMEM((32, 1, 128), F32),
                pltpu.VMEM((16, 16, 32), BF16),
                pltpu.VMEM((16, 4, 4, 512), F32),
                pltpu.VMEM((32, 256), F32),
                pltpu.SemaphoreType.DMA((16, 8)),
                pltpu.SemaphoreType.DMA((8,)),
                pltpu.SemaphoreType.DMA((2,)),
                pltpu.SemaphoreType.DMA((2,)),
                pltpu.SemaphoreType.DMA((4,)),
                pltpu.SemaphoreType.DMA((2,)),
                pltpu.SemaphoreType.DMA((6,)),
                pltpu.SemaphoreType.DMA,
                pltpu.SemaphoreType.DMA,
            ],
            compiler_params=pltpu.CompilerParams(has_side_effects=True, vmem_limit_bytes=40 * 1024 * 1024),
        )(wave_rows, left_rows, op_last, right_env)
        return vecs, alpha, beta

    return jax.shard_map(
        local_run, mesh=mesh,
        in_specs=(P("rows"), P(None, "rows"), P(), P()),
        out_specs=(P(None, "rows"), P(), P()), check_vma=False)
```

```python
import functools

import jax
import jax.numpy as jnp
from jax import lax
from jax.experimental import pallas as pl
from jax.experimental.pallas import tpu as pltpu
from jax.sharding import PartitionSpec as P

NUM_STEPS = 6
MESH = pl.DeviceIdType.MESH
F32 = jnp.float32
BF16 = jnp.bfloat16

ROUTES = ("zyx", "xzy", "zxy", "zyx", "zyx", "xzy", "zyx", "yxz")
ORDER = (
    "o3z", "o4y", "o0z", "o2y", "o1x", "o5y", "o1y", "o4z", "o2x", "o6x", "o2z", "o1z", "o7y", "o0y", "o7x", "o6z",
    "o3y", "o5x", "e3n1", "e0n1", "e2n1", "e1y0", "e1x0", "e2x0", "e7y0", "o6y", "e3n2", "e3y0", "e3x1", "e5y0",
    "e2n2", "o0x", "e7x0", "e0n2", "e3n3", "e5x0", "e4n1", "e0y0", "o3x", "e2n3", "e1x1", "e0n3", "e0y1", "e1n1",
    "o5z", "e3y2", "e3y3", "o7z", "e3d0", "e3x2", "e1x2", "e2x3", "e7d0", "e3y1", "e2x2", "e6y0", "e2y1", "e1n2",
    "e0y3", "e1x3", "e6x0", "e0y2", "e1n3", "e2x1", "e4n2", "e6n1", "e4n3", "e6n3", "e5d0", "e4y1", "e0d0", "e6n2",
    "e0x2", "e5n1", "e5x1", "e7d1", "e3x3", "e7x1", "e5n2", "e1d0", "e3d1", "e3d3", "e2y0", "e0d3", "e0x0", "e3d2",
    "e7y1", "e2d2", "e1d2", "e3x0", "l3", "e5x2", "e0x3", "e0d1", "e0x1", "e2d0", "e2y3", "e0d2", "o4x", "l0", "e7n1",
    "e2d3", "e1d3", "e1y3", "e2y2", "e7d2", "e1d1", "e6d0", "e1y1", "e1y2", "e2d1", "l2", "l1", "e5n3", "e4x3",
    "e4y3", "m0", "e4y0", "e4y2", "e7x2", "m1", "e6x3", "e6y1", "m2", "m3", "e7y2", "e5x3", "e6y3", "e6y2", "e7n2",
    "e6x1", "r0", "e4d1", "e4d3", "r1", "e5d1", "e4x2", "e4d2", "e7y3", "e7x3", "e4x1", "e7d3", "e4x0", "e4d0", "l4",
    "e7n3", "e5y3", "l7", "e5y2", "e6d1", "e5y1", "e6x2", "e5d2", "e5d3", "l5", "e6d2", "e6d3", "l6", "m4", "m5",
    "m6", "m7", "r2", "r3",
)


CLASSES = "nxyd"


def onward(route, cls, dist):
    if route[0] == "z":
        first, second = route[1], route[2]
    elif route[2] == "z":
        first, second = route[0], route[1]
    else:
        first, second = route[0], route[2]
    bit = {"x": 1, "y": 2}
    off_first, off_second = bool(cls & bit[first]), bool(cls & bit[second])
    if route[0] == "z":
        if cls == 0:
            return ["z", first, second]
        return [second] if off_first and not off_second else []
    if route[2] == "z":
        ways = []
        if dist == 0 and cls == 0:
            ways = [first, second]
        elif dist == 0 and off_first and not off_second:
            ways = [second]
        return ways + ["z"]
    if off_second:
        return []
    return ([first] if dist == 0 and not off_first else []) + [second, "z"]


def sends_on(way, cc, pz):
    count = 0
    for piece in range(4 * cc, 4 * cc + 4):
        for cls in range(4):
            for src_z in range(4):
                ways = onward(ROUTES[piece], cls, abs(pz - src_z))
                if way in ("x", "y"):
                    count += way in ways
                elif way == "up":
                    count += "z" in ways and src_z <= pz < 3
                else:
                    count += "z" in ways and src_z >= pz > 0
    return count


def lanczos_kernel(
    vec_count,
    psi_ref, left_ref, op_hbm, right_ref,
    out_ref, alpha_ref, beta_ref,
    u_ref, stage_ref, env_l, env_r, kron_ref, x_ref, y_ref, sig_ref, part_ref, v_ref, w_ref, stat_ref, op_ref, turn_ref, flat_ref,
    recv_sem, send_sem, pair_send, pair_recv, part_sem, stat_sem, load_sem, out_sem, psi_sem,
):
    idx = lax.axis_index("rows")
    core = lax.rem(idx, 2)
    pos_x = lax.rem(idx // 2, 2)
    pos_y = lax.rem(idx // 4, 2)
    pos_z = idx // 8
    chip = idx // 2
    sib = idx + 1 - 2 * core
    next_x = idx + 2 - 4 * pos_x
    next_y = idx + 4 - 8 * pos_y

    def block(piece, first_row, rows):
        return u_ref.at[piece // 4, pl.ds(2 * (piece % 4), 2), pl.ds(pl.multiple_of(first_row, 16), rows), :]

    WAYS = {"x": 0, "y": 1, "up": 2, "down": 3}

    def copy(piece, src, way, first_row, rows):
        target = {"x": next_x, "y": next_y, "up": idx + 8, "down": idx - 8}[way]
        ref = block(piece, first_row, rows)
        return pltpu.make_async_remote_copy(
            src_ref=ref, dst_ref=ref, send_sem=send_sem.at[WAYS[way] + 4 * (piece // 4)],
            recv_sem=recv_sem.at[src, piece], device_id=(target,), device_id_type=MESH)

    def send(piece, src, way, first_row=None, rows=32):
        if first_row is None:
            first_row = 32 * src
        if way == "up":
            @pl.when(pos_z < 3)
            def _():
                copy(piece, src, way, first_row, rows).start()
        elif way == "down":
            @pl.when(pos_z > 0)
            def _():
                copy(piece, src, way, first_row, rows).start()
        else:
            copy(piece, src, way, first_row, rows).start()

    def send_own(piece, way, first_row=None, rows=32):
        for one in (("up", "down") if way == "z" else (way,)):
            send(piece, chip, one, first_row, rows)

    def arrival(piece, cls, dist):
        col_x = 1 - pos_x if cls & 1 else pos_x
        col_y = 1 - pos_y if cls & 2 else pos_y

        def act(src_z, heading):
            src = (src_z * 2 + col_y) * 2 + col_x
            copy(piece, src, "x", 32 * src, 32).wait_recv()
            for way in onward(ROUTES[piece], cls, dist):
                if way != "z":
                    send(piece, src, way)
                else:
                    for one in heading:
                        send(piece, src, one)

        if dist == 0:
            act(pos_z, ("up", "down"))
            return

        @pl.when(pos_z >= dist)
        def _():
            act(pos_z - dist, ("up",))

        @pl.when(pos_z + dist <= 3)
        def _():
            act(pos_z + dist, ("down",))

    def sends_done():
        def wait(count, way, cc):
            if count:
                ref = env_r.at[0, pl.ds(0, count), pl.ds(0, 32), :]
                pltpu.make_async_copy(ref, ref, send_sem.at[WAYS[way] + 4 * cc]).wait()

        for cc in range(2):
            wait(sends_on("x", cc, 0), "x", cc)
            wait(sends_on("y", cc, 0), "y", cc)
        for pz in range(4):
            @pl.when(pos_z == pz)
            def _():
                for cc in range(2):
                    wait(sends_on("up", cc, pz), "up", cc)
                    wait(sends_on("down", cc, pz), "down", cc)

    my_rows = pl.ds(pl.multiple_of(32 * chip + 16 * core, 16), 16)
    right_loads = [
        pltpu.make_async_copy(
            right_ref.at[:, pl.ds(pl.multiple_of(256 * core + 128 * cc, 128), 128), :], env_r.at[cc], load_sem.at[cc])
        for cc in range(2)]
    left_load = pltpu.make_async_copy(left_ref, env_l.at[:, core], load_sem.at[2])
    left_send = pltpu.make_async_remote_copy(
        src_ref=left_ref, dst_ref=env_l.at[:, core], send_sem=load_sem.at[3], recv_sem=load_sem.at[4],
        device_id=(sib,), device_id_type=MESH)
    left_send.start()
    left_load.start()
    psi_loads = [
        pltpu.make_async_copy(psi_ref.at[:, q // 4, q % 4, :], w_ref.at[pl.ds(16 * q, 16), :], psi_sem) for q in range(16)]
    for load in psi_loads:
        load.start()
    op_load = pltpu.make_async_copy(op_hbm, op_ref, load_sem.at[5])
    op_load.start()
    for load in right_loads:
        load.start()

    def build_kron():
        big_row = lax.broadcasted_iota(jnp.int32, (256, 256), 0)
        big_col = lax.broadcasted_iota(jnp.int32, (256, 256), 1)
        row_hi, row_lo = lax.shift_right_logical(big_row, 4), big_row & 15
        col_hi, col_lo = lax.shift_right_logical(big_col, 4), big_col & 15
        spread = jnp.where(row_lo == col_hi, 1.0, 0.0).astype(BF16)
        flat_ref[...] = jnp.transpose(op_ref[...].reshape(256, 32).astype(F32))

        def some(k8, carry):
            for kk in range(8):
                k = k8 * 8 + kk
                tall = jnp.where(row_hi == col_hi, flat_ref[pl.ds(k, 1), :], 0.0).astype(BF16)
                full = jnp.dot(tall, spread, preferred_element_type=F32)
                kron_ref[k] = jnp.where(row_lo == col_lo, full, 0.0).astype(BF16)
            return carry

        lax.fori_loop(0, 4, some, 0)

    def left_part(piece):
        for sub in range(2):
            rp = 2 * (piece % 4) + sub
            out = jnp.dot(env_l[...].reshape(1024, 512), u_ref[piece // 4, rp], preferred_element_type=F32)
            out = out.astype(BF16).reshape(32, 2, 16, 256)
            for ag in range(2):
                for par in range(2):
                    row = (2 * rp + par) * 16
                    x_ref[:, row:row + 16, ag * 128:(ag + 1) * 128] = out[:, ag, :, par * 128:(par + 1) * 128]

    def mid_part(part):
        for kk in range(8):
            k = 8 * (part % 4) + kk
            out = jnp.dot(kron_ref[k], x_ref[k], preferred_element_type=F32).astype(BF16)
            for ag in range(2):
                y_ref[ag, :, k * 128:(k + 1) * 128] = out[:, ag * 128:(ag + 1) * 128]

    def right_part(part):
        cc, who = part // 2, part % 2
        ag = 1 - core if who == 0 else core
        out = jnp.dot(y_ref[ag], env_r[cc].reshape(4096, 512), preferred_element_type=F32)
        sig_ref[who] = out if cc == 0 else sig_ref[who] + out

    def right_half(half):
        lanes = slice(256 * half, 256 * half + 256)
        rhs = env_r[1, :, :, lanes].reshape(4096, 256)
        sig_ref[0, :, lanes] = sig_ref[0, :, lanes] + jnp.dot(y_ref[1 - core], rhs, preferred_element_type=F32)

    lane = lax.broadcasted_iota(jnp.int32, (1, 128), 1)

    def total(val):
        cols = val.shape[1]
        part = val[:, 0:128]
        for first in range(128, cols, 128):
            part = part + val[:, first:first + 128]
        return jnp.sum(jnp.sum(part, axis=0, keepdims=True), axis=1, keepdims=True)

    def start_stats(dot_val, proj, sq_w, sq_v, cross):
        row = jnp.where(lane == 0, dot_val, 0.0)
        for which, val in ((1, proj), (2, sq_w), (3, sq_v), (4, cross)):
            row = jnp.where(lane == which, val, row)
        stat_ref[idx] = row

        flips = [(1 - pos_x if m & 2 else pos_x) * 2 + (1 - core if m & 1 else core) for m in range(4)]
        flips += [flip + 4 * (1 - pos_y) for flip in flips[:4]]
        flips = [flip + 4 * pos_y for flip in flips[:4]] + flips[4:]
        z_low, z_high = lax.rem(pos_z, 2), pos_z // 2
        for m in range(31, 0, -1):
            high = 1 - z_high if m & 16 else z_high
            low = 1 - z_low if m & 8 else z_low
            pltpu.make_async_remote_copy(
                src_ref=stat_ref.at[idx], dst_ref=stat_ref.at[idx], send_sem=stat_sem.at[0], recv_sem=stat_sem.at[1],
                device_id=(16 * high + 8 * low + flips[m % 8],), device_id_type=MESH).start()

    def finish_stats():
        others = stat_ref.at[pl.ds(0, 31)]
        pltpu.make_async_copy(others, others, stat_sem.at[1]).wait()
        pltpu.make_async_copy(others, others, stat_sem.at[0]).wait()

        def pick(row, which):
            return jnp.sum(jnp.where(lane == which, row, 0.0), axis=1, keepdims=True)

        rows = [stat_ref[d] for d in range(32)]
        whole = rows[0]
        for row in rows[1:]:
            whole = whole + row
        alpha = pick(whole, 0) / vec_count
        extra = jnp.zeros((1, 128), F32)
        for row in rows:
            delta = alpha - pltpu.roll(row, 2, 1)
            extra = extra + delta * (delta * row - 2.0 * pltpu.roll(row, 127, 1))
        beta_sq = jnp.sum(jnp.where(lane == 2, whole, jnp.where(lane == 3, extra, 0.0)), axis=1, keepdims=True)
        return alpha, jnp.sqrt(beta_sq / vec_count)

    def fold(val):
        return val[0:8] + val[8:16]

    def normalise(slot, prev, alpha, beta, proj, keep):
        delta = alpha - proj
        scale = 1.0 / beta
        acc = jnp.zeros((8, 512), F32)
        for q in range(16):
            rows = pl.ds(16 * q, 16)
            vec = (w_ref[rows, :] - delta * v_ref[prev, rows, :]) * scale
            v_ref[slot, rows, :] = vec
            acc = acc + fold(vec * vec)
            keep(q, vec)
        return acc

    def turn(slot):
        for q in range(16):
            turn_ref[:, q // 4, q % 4, :] = v_ref[slot, pl.ds(16 * q, 16), :]

    def out_copy(step):
        return pltpu.make_async_copy(turn_ref, out_ref.at[step], out_sem)

    for load in psi_loads:
        load.wait()
    acc = jnp.zeros((8, 512), F32)
    for q in range(16):
        rows = pl.ds(16 * q, 16)
        acc = acc + fold(w_ref[rows, :] * w_ref[rows, :])
        v_ref[1, rows, :] = jnp.zeros((16, 512), F32)
        v_ref[2, rows, :] = jnp.zeros((16, 512), F32)
    nought = jnp.zeros((1, 1), F32)
    start_stats(nought, nought, total(acc), nought, nought)
    op_load.wait()
    build_kron()

    def step_body(j, proj):
        cur = lax.rem(j, 3)
        prev = lax.rem(j + 2, 3)
        alpha, beta = finish_stats()

        def to_bf16(q, vec):
            low, high = vec[:, 0:256], vec[:, 256:512]
            own = jnp.where(core == 0, low, high).astype(BF16)
            far = jnp.where(core == 0, high, low).astype(BF16)
            lanes = slice(q % 2 * 128, q % 2 * 128 + 128)
            for cc in range(2):
                u_ref[cc, q // 2, my_rows, lanes] = own[:, cc * 128:(cc + 1) * 128]
                stage_ref[cc, q // 2, :, lanes] = far[:, cc * 128:(cc + 1) * 128]

        acc_v = normalise(cur, prev, alpha, beta, proj, to_bf16)

        def pair_copy(cc):
            return pltpu.make_async_remote_copy(
                src_ref=stage_ref.at[cc], dst_ref=u_ref.at[cc, :, my_rows, :],
                send_sem=pair_send.at[cc], recv_sem=pair_recv.at[cc], device_id=(sib,), device_id_type=MESH)

        for cc in range(2):
            pair_copy(cc).start()
        lead = 0
        while ORDER[lead][0] == "o":
            lead += 1
        for word in ORDER[:lead]:
            send_own(int(word[1]), word[2], 32 * chip + 16 * core, 16)
        sq_v = total(acc_v)

        @pl.when(j > 0)
        def _():
            alpha_ref[j - 1] = alpha[0, 0]
            beta_ref[j - 1] = beta[0, 0]
            out_copy(j - 1).wait()

        turn(cur)
        out_copy(j).start()
        for cc in range(2):
            pair_copy(cc).wait_recv()
            for word in ORDER[:lead]:
                if int(word[1]) // 4 == cc:
                    send_own(int(word[1]), word[2], 32 * chip + 16 * (1 - core), 16)

        def part_copy(half):
            lanes = slice(256 * half, 256 * half + 256)
            return pltpu.make_async_remote_copy(
                src_ref=sig_ref.at[0, :, lanes], dst_ref=part_ref.at[:, lanes],
                send_sem=part_sem.at[half], recv_sem=part_sem.at[2 + half], device_id=(sib,), device_id_type=MESH)

        loaded = False
        for word in ORDER[lead:]:
            what, piece = word[0], int(word[1])
            if what == "o":
                send_own(piece, word[2])
            elif what == "e":
                arrival(piece, CLASSES.index(word[2]), int(word[3]))
            elif what == "l":
                if not loaded:
                    loaded = True

                    @pl.when(j == 0)
                    def _():
                        left_load.wait()
                        left_send.wait()
                        for load in right_loads:
                            load.wait()
                left_part(piece)
            elif what == "m":
                mid_part(piece)
            else:
                right_part(piece)
                if piece == 2:
                    for half in range(2):
                        part_copy(half).start()
        for cc in range(2):
            pair_copy(cc).wait_send()
        sends_done()
        for half in range(2):
            part_copy(half).wait()
        acc_p = jnp.zeros((8, 512), F32)
        for q in range(16):
            rows = pl.ds(16 * q, 16)
            sig = sig_ref[1, rows, :] + part_ref[rows, :]
            w_ref[rows, :] = sig
            acc_p = acc_p + fold(sig * v_ref[cur, rows, :])
        dot_val = total(acc_p)
        new_proj = jnp.where(sq_v > 0.0, dot_val / jnp.where(sq_v > 0.0, sq_v, 1.0), 0.0)
        beta_use = jnp.where(j > 0, beta, 0.0)
        acc_w = jnp.zeros((8, 512), F32)
        acc_c = jnp.zeros((8, 512), F32)
        for q in range(16):
            rows = pl.ds(16 * q, 16)
            vec = v_ref[cur, rows, :]
            res = w_ref[rows, :] - beta_use * v_ref[prev, rows, :] - new_proj * vec
            w_ref[rows, :] = res
            acc_w = acc_w + fold(res * res)
            acc_c = acc_c + fold(res * vec)
        start_stats(dot_val, new_proj, total(acc_w), sq_v, total(acc_c))
        return new_proj

    proj = lax.fori_loop(0, NUM_STEPS, step_body, nought)
    alpha, beta = finish_stats()
    last = NUM_STEPS % 3
    normalise(last, (NUM_STEPS - 1) % 3, alpha, beta, proj, lambda q, vec: None)
    out_copy(NUM_STEPS - 1).wait()
    turn(last)
    out_copy(NUM_STEPS).start()
    alpha_ref[NUM_STEPS - 1] = alpha[0, 0]
    beta_ref[NUM_STEPS - 1] = beta[0, 0]
    out_copy(NUM_STEPS).wait()


def solution(mesh):
    def local_run(wave_rows, left_rows, op_pair, right_env):
        rows, phys, _, bond = wave_rows.shape
        pair = phys * phys
        vec_count = float(bond * bond * pair)
        op_last = jnp.transpose(op_pair, (1, 2, 0))
        vecs, alpha, beta = pl.pallas_call(
            functools.partial(lanczos_kernel, vec_count),
            out_shape=(
                jax.ShapeDtypeStruct((NUM_STEPS + 1, rows, phys, phys, bond), F32),
                jax.ShapeDtypeStruct((NUM_STEPS,), F32),
                jax.ShapeDtypeStruct((NUM_STEPS,), F32),
            ),
            in_specs=[pl.BlockSpec(memory_space=pl.ANY)] * 4,
            out_specs=(
                pl.BlockSpec(memory_space=pl.ANY),
                pl.BlockSpec(memory_space=pltpu.SMEM),
                pl.BlockSpec(memory_space=pltpu.SMEM),
            ),
            scratch_shapes=[
                pltpu.VMEM((2, 8, 512, 256), BF16),
                pltpu.VMEM((2, 8, 16, 256), BF16),
                pltpu.VMEM((32, 2, 16, 512), BF16),
                pltpu.VMEM((2, 32, 128, 512), BF16),
                pltpu.VMEM((32, 256, 256), BF16),
                pltpu.VMEM((32, 256, 256), BF16),
                pltpu.VMEM((2, 256, 4096), BF16),
                pltpu.VMEM((2, 256, 512), F32),
                pltpu.VMEM((256, 512), F32),
                pltpu.VMEM((3, 256, 512), F32),
                pltpu.VMEM((256, 512), F32),
                pltpu.VMEM((32, 1, 128), F32),
                pltpu.VMEM((16, 16, 32), BF16),
                pltpu.VMEM((16, 4, 4, 512), F32),
                pltpu.VMEM((32, 256), F32),
                pltpu.SemaphoreType.DMA((16, 8)),
                pltpu.SemaphoreType.DMA((8,)),
                pltpu.SemaphoreType.DMA((2,)),
                pltpu.SemaphoreType.DMA((2,)),
                pltpu.SemaphoreType.DMA((4,)),
                pltpu.SemaphoreType.DMA((2,)),
                pltpu.SemaphoreType.DMA((6,)),
                pltpu.SemaphoreType.DMA,
                pltpu.SemaphoreType.DMA,
            ],
            compiler_params=pltpu.CompilerParams(has_side_effects=True, vmem_limit_bytes=40 * 1024 * 1024),
        )(wave_rows, left_rows, op_last, right_env)
        return vecs, alpha, beta

    return jax.shard_map(
        local_run, mesh=mesh,
        in_specs=(P("rows"), P(None, "rows"), P(), P()),
        out_specs=(P(None, "rows"), P(), P()), check_vma=False)
```
